512 devices in a mesh: gx: 16 (over z_hi, y, core), gy: 32 (over z_lo, x).
Axes of the slice: x: 4, y: 4, z: 16 (z_hi: 2, z_lo: 8; z = z_hi * 8 + z_lo), core: 2. Of those that a mesh axis runs over, the one named last changes fastest.
Arguments:
- particle_cell: int32 [16, 32, 65536], P('gx', 'gy'), may hold values from -1 to 16383, as said below
- particle_mass: float32 [16, 32, 65536], P('gx', 'gy'), may hold values from 0.5 to 2
Outputs:
- potential: float32 [256, 256, 128], P('gx', 'gy')
- residual: float32 [256, 256, 128], P('gx', 'gy')
- residual_norms: float32 [2], replicated
The draws below stay inside these ranges and needn't reach their ends.
Inputs may be any that keep to these rules, and one draw needn't show every extreme that they name: `particle_cell`: -1 marks an empty slot; any other value v names the cell (v // 1024, v // 128 % 8, v % 128) of the block of 16 x 8 x 128 cells that belongs to the slot's tile.
All inputs are finite; a program needn't handle non-finite values.
Results may differ from the reference program's by a relative error of at most 0.0003.
Values sent between devices are 32-bit elements; how exact they have to be, the bound alone decides.
No kernel may reach another device: no remote copies, remote signals or barrier semaphores. Data moves between devices by JAX's collectives and lax.ppermute only.
A program may use at most 64 MiB of HBM per device.

```python
import math
import jax
import jax.numpy as jnp

CX = 16
CY = 8
NZ = 128
P_DEV = 65536
LEVELS = 4
CYCLES = 2
COARSE_SWEEPS = 2
TILES_X = 16
TILES_Y = 32
NX = 256
NY = 256


def shuffled_ranks(subkey):
    return jax.random.permutation(subkey, P_DEV)


def draw_particle_cell(key, part):
    tile_count = TILES_X * TILES_Y
    block_cells = CX * CY * NZ
    base = jax.random.fold_in(key, 11)
    key_cell, key_keep, key_jitter = jax.random.split(base, 3)
    placed = jax.random.randint(key_cell, (tile_count, P_DEV), 0, block_cells, dtype=jnp.int32)
    order = jnp.arange(tile_count, dtype=jnp.int32)
    span_tiles = max(tile_count - 1, 1)
    occupied_count = P_DEV - 2 * P_DEV // 3 * (tile_count - 1 - order) // span_tiles
    jitter = jax.random.randint(key_jitter, (tile_count,), 0, P_DEV // 8 + 1, dtype=jnp.int32)
    occupied_count = occupied_count - jnp.where(order == tile_count - 1, 0, jitter)
    ranks = jax.vmap(shuffled_ranks)(jax.random.split(key_keep, tile_count)).astype(jnp.int32)
    chosen = jnp.where(ranks < occupied_count[:, None], placed, -1)
    return chosen.reshape(TILES_X, TILES_Y, P_DEV).astype(jnp.int32)


def shard_levels(key, shape, shards, smallest, largest):
    gain, own = 1.0, jax.random.fold_in(key, 6)
    for position, shards_of in shards:
        heights = jnp.exp(jax.random.uniform(jax.random.fold_in(own, position), (shards_of,), jnp.float32, smallest / len(shards), largest / len(shards)))
        gain = gain * jnp.repeat(heights, shape[position] // shards_of).reshape([-1 if axis == position else 1 for axis in range(len(shape))])
    return gain


def setup_inputs(seed: int = 0) -> dict:
    streams_of = jax.random.split(jax.random.key(seed), 3)
    particle_cell = draw_particle_cell(jax.random.fold_in(streams_of[2], 71), 0)
    particle_mass = jnp.clip(jnp.exp(math.log(2.0) - 1.3862944 * jax.random.uniform(streams_of[1], (TILES_X, TILES_Y, P_DEV), jnp.float32) ** shard_levels(streams_of[1], (TILES_X, TILES_Y, P_DEV), ((0, 16), (1, 32)), -0.2, 0.2)), 0.5, 2.0)
    return {"particle_cell": particle_cell, "particle_mass": particle_mass}


coupling = 0.03125
norm_eps = 1e-06

def roll_sum(values):
    beside = jnp.roll(values, 1, 0) + jnp.roll(values, -1, 0)
    beside = beside + jnp.roll(values, 1, 1) + jnp.roll(values, -1, 1)
    return beside + jnp.roll(values, 1, 2) + jnp.roll(values, -1, 2)

def parity_mask(shape):
    index_x = jnp.arange(shape[0], dtype=jnp.int32)[:, None, None]
    index_y = jnp.arange(shape[1], dtype=jnp.int32)[None, :, None]
    index_z = jnp.arange(shape[2], dtype=jnp.int32)[None, None, :]
    return (index_x + index_y + index_z) % 2 == 0

def whole_sweep(estimate, source, spacing_squared, red_cells):
    updated = (roll_sum(estimate) + spacing_squared * source) / 6.0
    estimate = jnp.where(red_cells, updated, estimate)
    updated = (roll_sum(estimate) + spacing_squared * source) / 6.0
    return jnp.where(red_cells, estimate, updated)

def whole_residual(estimate, source, spacing_squared):
    return source - (6.0 * estimate - roll_sum(estimate)) / spacing_squared

def restrict(values):
    rows_x, rows_y, rows_z = values.shape
    return values.reshape(rows_x // 2, 2, rows_y // 2, 2, rows_z // 2, 2).mean(axis=(1, 3, 5))

def prolong(values):
    rows_x, rows_y, rows_z = values.shape
    spread = jnp.broadcast_to(values[:, None, :, None, :, None], (rows_x, 2, rows_y, 2, rows_z, 2))
    return spread.reshape(2 * rows_x, 2 * rows_y, 2 * rows_z)

def whole_cycle(grid_level, estimate, source):
    spacing_squared = float(4 ** grid_level)
    red_cells = parity_mask(estimate.shape)
    if grid_level == LEVELS - 1:
        for repeat in range(COARSE_SWEEPS):
            estimate = whole_sweep(estimate, source, spacing_squared, red_cells)
        return estimate
    estimate = whole_sweep(estimate, source, spacing_squared, red_cells)
    coarse_source = restrict(whole_residual(estimate, source, spacing_squared))
    correction = whole_cycle(grid_level + 1, jnp.zeros_like(coarse_source), coarse_source)
    estimate = estimate + prolong(correction)
    return whole_sweep(estimate, source, spacing_squared, red_cells)

def reference(particle_cell, particle_mass):
    grid_cells = NX * NY * NZ
    local_x = particle_cell // (CY * NZ)
    local_y = particle_cell // NZ % CY
    local_z = particle_cell % NZ
    tile_x = jnp.arange(TILES_X, dtype=jnp.int32)[:, None, None]
    tile_y = jnp.arange(TILES_Y, dtype=jnp.int32)[None, :, None]
    flat_index = ((tile_x * CX + local_x) * NY + tile_y * CY + local_y) * NZ + local_z
    occupied = particle_cell >= 0
    flat_index = jnp.where(occupied, flat_index, grid_cells).astype(jnp.int32)
    density = jnp.zeros((grid_cells + 1,), jnp.float32).at[flat_index.reshape(-1)].add(particle_mass.reshape(-1))
    density = density[:grid_cells].reshape(NX, NY, NZ)
    total_mass = jnp.sum(jnp.where(occupied, particle_mass, 0.0))
    mean_mass = total_mass / grid_cells
    source = coupling * (1.0 - density / mean_mass)
    estimate = jnp.zeros((NX, NY, NZ), jnp.float32)
    norm_list = []
    residual = source
    for cycle_index in range(CYCLES):
        estimate = whole_cycle(0, estimate, source)
        residual = whole_residual(estimate, source, 1.0) / coupling
        norm_list.append(jnp.sqrt(jnp.sum(residual * residual) / grid_cells + norm_eps))
    return (estimate, residual, jnp.stack(norm_list))
```

```python
import functools

import jax
import jax.numpy as jnp
from jax import lax
from jax.experimental import pallas as pl
from jax.experimental.pallas import tpu as pltpu
from jax.sharding import Mesh
from jax.sharding import PartitionSpec as P

CX = 16
CY = 8
NZ = 128
GX = ("gx_0", "gx_1", "gx_2")
GY = ("gy_0", "gy_1")
Z_RING = ("gx_0", "gy_0")
PLANE = ("gx_1", "gx_2", "gy_1")
TILES_X = 16
TILES_Y = 32
GRID_CELLS = 256 * 256 * 128
COARSE_CELLS = 64 * 64 * 32

coupling = 0.03125
norm_eps = 1e-06

W0X, W0Y = 64, 56
W1X, W1Y = 32, 32
W2X, W2Y = 36, 40
W3X, W3Y = 18, 24
VMEM = pltpu.VMEM


def deposit_kernel(cell_ref, mass_ref, out_ref):
    rows = lax.broadcasted_iota(jnp.int32, (128, 128), 0)

    def step(t, acc):
        cells = cell_ref[pl.ds(pl.multiple_of(t * 8, 8), 8), :]
        masses = mass_ref[pl.ds(pl.multiple_of(t * 8, 8), 8), :]
        high = cells >> 7
        low = cells & 127
        coarse = masses.astype(jnp.bfloat16).astype(jnp.float32)
        fine = masses - coarse
        left, right = [], []
        for r in range(8):
            hit = rows == high[r : r + 1, :]
            first = jnp.where(hit, coarse[r : r + 1, :], 0.0).astype(jnp.bfloat16)
            second = jnp.where(hit, fine[r : r + 1, :], 0.0).astype(jnp.bfloat16)
            left.append(jnp.concatenate([first, second], axis=0))
            right.append(jnp.where(rows == low[r : r + 1, :], 1.0, 0.0).astype(jnp.bfloat16))
        left = jnp.concatenate(left, axis=1)
        right = jnp.concatenate(right, axis=1)
        return acc + lax.dot_general(left, right, (((1,), (1,)), ((), ())), preferred_element_type=jnp.float32)

    total = lax.fori_loop(0, cell_ref.shape[0] // 8, step, jnp.zeros((256, 128), jnp.float32))
    out_ref[...] = total[:128] + total[128:]


def row_parity(rows, lanes_per_cell, extra=0):
    j = lax.broadcasted_iota(jnp.int32, (rows, NZ), 0)
    z = lax.broadcasted_iota(jnp.int32, (rows, NZ), 1) // lanes_per_cell
    return (j + z + extra) & 1


def around(ref, i, rows, lanes):
    c = ref[i]
    n = ref[i - 1] + ref[i + 1]
    n = n + (pltpu.roll(c, 1, 0) + pltpu.roll(c, rows - 1, 0))
    return c, n + (pltpu.roll(c, lanes, 1) + pltpu.roll(c, NZ - lanes, 1))


def pair_z(t, lanes):
    z = lax.broadcasted_iota(jnp.int32, t.shape, 1) // lanes
    return t + jnp.where((z & 1) == 0, pltpu.roll(t, NZ - lanes, 1), pltpu.roll(t, lanes, 1))


def loop(lo, hi, body, unroll=2):
    def step(i, carry):
        body(i)
        return carry

    lax.fori_loop(lo, hi, step, 0, unroll=unroll)


def first_sweep(u, b, parity, rows, lanes, s, lo, hi):
    def body(i):
        c, n = around(b, i, rows, lanes)
        red = parity == (i & 1)
        u[i] = jnp.where(red, c * (s / 6.0), n * (s / 36.0) + c * (s / 6.0))

    loop(lo, hi, body)


def half_sweep(u, get_b, parity, colour, rows, lanes, s, lo, hi):
    def body(i):
        c, n = around(u, i, rows, lanes)
        chosen = parity == ((i + colour) & 1)
        u[i] = jnp.where(chosen, (n + s * get_b(i)) * (1.0 / 6.0), c)

    loop(lo, hi, body)


def residual_at(u, b, i, rows, lanes, s):
    c, n = around(u, i, rows, lanes)
    return b - (6.0 * c - n) * (1.0 / s)


def restrict_to(out, u, get_b, rows, lanes, s, lo, hi, scr, out_rows):
    def body(p):
        t = residual_at(u, get_b(2 * p), 2 * p, rows, lanes, s)
        t = t + residual_at(u, get_b(2 * p + 1), 2 * p + 1, rows, lanes, s)
        scr[0:rows, :] = pair_z(t, lanes)
        out[p] = (scr[pl.ds(0, out_rows, 2), :] + scr[pl.ds(1, out_rows, 2), :]) * 0.125

    loop(lo, hi, body, 1)


def spread_rows(value, rows, scr):
    scr[pl.ds(0, rows, 2), :] = value
    scr[pl.ds(1, rows, 2), :] = value
    return scr[0 : 2 * rows, :]


def own_coarse(u1, b1, send_ref):
    lane = lax.broadcasted_iota(jnp.int32, (W1Y, NZ), 1) & 3
    packed = jnp.zeros((W1Y, NZ), jnp.float32)
    for x in range(4):
        i = 12 + 2 * x
        t = residual_at(u1, b1[i], i, W1Y, 2, 4.0) + residual_at(u1, b1[i + 1], i + 1, W1Y, 2, 4.0)
        t = pair_z(t, 2)
        t = (t + pltpu.roll(t, W1Y - 1, 0)) * 0.125
        packed = jnp.where(lane == x, t, packed)
    for k in range(send_ref.shape[0]):
        send_ref[k, 0:1, :] = packed[12:13, :]
        send_ref[k, 1:2, :] = packed[14:15, :]


def coarse_solve(pos_ref, ag, shift, pw, b2, u2, b3, u3, scr):
    gx, gy = pos_ref[0], pos_ref[1]
    pw[...] = jnp.zeros(pw.shape, jnp.float32)
    for tx in range(9):
        x = lax.rem(gx + (tx - 4 + TILES_X), TILES_X)
        for ty in range(17):
            y = lax.rem(gy + (ty - 8 + TILES_Y), TILES_Y)
            plane = (x & 7) * 4 + (y & 3)
            ring = (x >> 3) * 8 + (y >> 2)
            pw[tx, 2 * ty : 2 * ty + 2, :] = ag[plane * 16 + ring]
    lane = lax.broadcasted_iota(jnp.int32, (W2Y, NZ), 1) & 3

    def unpack(tx):
        t = pw[tx]
        for j in range(4):
            v = jnp.where(lane == j, t, 0.0)
            v = v + pltpu.roll(v, 1 if j % 2 == 0 else NZ - 1, 1)
            v = v + pltpu.roll(v, 2 if j < 2 else NZ - 2, 1)
            b2[4 * tx + j] = v - shift

    loop(0, 9, unpack, 1)
    par2 = row_parity(W2Y, 4)
    u2[0] = jnp.zeros((W2Y, NZ), jnp.float32)
    u2[W2X - 1] = jnp.zeros((W2Y, NZ), jnp.float32)
    first_sweep(u2, b2, par2, W2Y, 4, 16.0, 1, W2X - 1)
    scr[32:64, :] = jnp.zeros((32, NZ), jnp.float32)
    for i in (0, W3X - 1):
        b3[i] = jnp.zeros((W3Y, NZ), jnp.float32)
        u3[i] = jnp.zeros((W3Y, NZ), jnp.float32)
    restrict_to(b3, u2, lambda i: b2[i], W2Y, 4, 16.0, 1, W3X - 1, scr, W3Y)
    par3 = row_parity(W3Y, 8, gy)
    first_sweep(u3, b3, par3, W3Y, 8, 64.0, 1, W3X - 1)
    for colour in (0, 1):
        half_sweep(u3, lambda i: b3[i], par3, colour, W3Y, 8, 64.0, 1, W3X - 1)

    def add(p):
        c = spread_rows(u3[p], W3Y, scr)[0:W2Y]
        u2[2 * p] = u2[2 * p] + c
        u2[2 * p + 1] = u2[2 * p + 1] + c

    loop(4, 14, add, 1)
    half_sweep(u2, lambda i: b2[i], par2, 0, W2Y, 4, 16.0, 9, 27)
    half_sweep(u2, lambda i: b2[i], par2, 1, W2Y, 4, 16.0, 10, 26)


def up_level1(v1, u1, b1, shift, u2, scr):
    def add(p):
        c = spread_rows(u2[p + 10, 10:26, :], 16, scr)
        v1[2 * p] = u1[2 * p] - shift * (4.0 / 3.0) + c
        v1[2 * p + 1] = u1[2 * p + 1] - shift * (4.0 / 3.0) + c

    loop(0, 16, add, 1)
    par1 = row_parity(W1Y, 2)
    for colour in (0, 1):
        half_sweep(v1, lambda i: b1[i] - shift, par1, colour, W1Y, 2, 4.0, 1, W1X - 1)


def up_level0(v0, u0, d, shift, base, v1, scr, lo, hi):
    def add(p):
        c = spread_rows(v1[p], W1Y, scr)[0:W0Y]
        v0[2 * p] = u0[2 * p] - base + c
        v0[2 * p + 1] = u0[2 * p + 1] - base + c

    loop(lo // 2, hi // 2, add, 1)
    par0 = row_parity(W0Y, 1)
    for colour in (0, 1):
        half_sweep(v0, lambda i: d[i] - shift, par0, colour, W0Y, 1, 1.0, lo + 1, hi - 1)


def down_level1(u1, b1, send_ref):
    u1[0] = jnp.zeros((W1Y, NZ), jnp.float32)
    u1[W1X - 1] = jnp.zeros((W1Y, NZ), jnp.float32)
    first_sweep(u1, b1, row_parity(W1Y, 2), W1Y, 2, 4.0, 1, W1X - 1)
    own_coarse(u1, b1, send_ref)


def pre_kernel(pos_ref, x_ref, p1e, p1o, p2a, p2b, p3a, p3b, send_ref, d, u0, b1, u1, scr):
    gy = pos_ref[1]
    d[:, 24:32, :] = x_ref[...]

    def place(first, second, offset):
        d[:, 24 + offset : 32 + offset, :] = first[...]
        d[:, 24 - offset : 32 - offset, :] = second[...]

    even = (gy & 1) == 0
    low = (gy & 3) < 2
    for cond, a, b, offset in ((even, p1e, p1o, 8), (low, p2a, p2b, 16), (even, p3a, p3b, 24)):
        pl.when(cond)(functools.partial(place, a, b, offset))
        pl.when(jnp.logical_not(cond))(functools.partial(place, b, a, offset))
    for i in (0, W0X - 1):
        u0[i] = jnp.zeros((W0Y, NZ), jnp.float32)
    first_sweep(u0, d, row_parity(W0Y, 1), W0Y, 1, 1.0, 1, W0X - 1)
    scr[...] = jnp.zeros(scr.shape, jnp.float32)
    for i in (0, W1X - 1):
        b1[i] = jnp.zeros((W1Y, NZ), jnp.float32)
    restrict_to(b1, u0, lambda i: d[i], W0Y, 1, 1.0, 1, W1X - 1, scr, W1Y)
    down_level1(u1, b1, send_ref)


def own_squares(u, d, shift):
    total = jnp.zeros((CY, NZ), jnp.float32)
    for i in range(24, 40):
        r = residual_at(u, d[i] - shift, i, W0Y, 1, 1.0)[24:32]
        total = total + r * r
    return total


def mid_kernel(pos_ref, ag, d, u0, b1, u1, send_ref, u0n, b1n, u1n, stat_ref, v1, pw, b2, u2, b3, u3, scr):
    total = jnp.sum(jnp.sum(ag[...], axis=0))
    mean = total * (1.0 / COARSE_CELLS)
    coarse_solve(pos_ref, ag, mean, pw, b2, u2, b3, u3, scr)
    up_level1(v1, u1, b1, mean, u2, scr)
    up_level0(u0n, u0, d, mean, mean * (1.0 / 3.0), v1, scr, 0, W0X)
    stat_ref[0:8, :] = own_squares(u0n, d, mean)
    stat_ref[8:16, :] = jnp.full((8, NZ), mean, jnp.float32)
    par0 = row_parity(W0Y, 1)
    for colour in (0, 1):
        half_sweep(u0n, lambda i: d[i] - mean, par0, colour, W0Y, 1, 1.0, 8, 56)
    scr[...] = jnp.zeros(scr.shape, jnp.float32)
    for i in range(W1X):
        if i < 6 or i >= 26:
            b1n[i] = jnp.zeros((W1Y, NZ), jnp.float32)
    restrict_to(b1n, u0n, lambda i: d[i] - mean, W0Y, 1, 1.0, 6, 26, scr, W1Y)
    down_level1(u1n, b1n, send_ref)


def post_kernel(pos_ref, ag, d, u0, b1, u1, stat, pot_ref, res_ref, sums_ref, v0, v1, pw, b2, u2, b3, u3, scr):
    mean = jnp.max(stat[8:16, :])
    coarse_solve(pos_ref, ag, 0.0, pw, b2, u2, b3, u3, scr)
    up_level1(v1, u1, b1, 0.0, u2, scr)
    up_level0(v0, u0, d, mean, 0.0, v1, scr, 16, 48)
    inv = 1.0 / jnp.full((CY, NZ), mean, jnp.float32)
    total = jnp.zeros((CY, NZ), jnp.float32)
    for i in range(16):
        r = residual_at(v0, d[24 + i] - mean, 24 + i, W0Y, 1, 1.0)[24:32] * inv
        total = total + r * r
        res_ref[i] = -r
        pot_ref[i] = v0[24 + i, 24:32, :] * (-coupling * inv)
    first = stat[0:8, :] * (inv * inv)
    lane = lax.broadcasted_iota(jnp.int32, (1, NZ), 1)
    both = jnp.where(lane == 0, jnp.sum(first), 0.0) + jnp.where(lane == 1, jnp.sum(total), 0.0)
    for k in range(sums_ref.shape[0]):
        sums_ref[k] = both


def f32(*shape):
    return jax.ShapeDtypeStruct(shape, jnp.float32)


def vmem(*shape):
    return pltpu.VMEM(shape, jnp.float32)


COARSE_SCRATCH = (vmem(9, W2Y, NZ), vmem(W2X, W2Y, NZ), vmem(W2X, W2Y, NZ), vmem(W3X, W3Y, NZ), vmem(W3X, W3Y, NZ), vmem(64, NZ))
LEVELS_OUT = (f32(W0X, W0Y, NZ), f32(W1X, W1Y, NZ), f32(W1X, W1Y, NZ))


def call(kernel, outs, scratch, *args, pos=None):
    whole = pl.BlockSpec(memory_space=VMEM)
    specs = [whole] * len(args)
    if pos is not None:
        specs = [pl.BlockSpec(memory_space=pltpu.SMEM)] + specs
        args = (pos, *args)
    return pl.pallas_call(
        kernel,
        out_shape=outs,
        in_specs=specs,
        out_specs=jax.tree.map(lambda _: whole, outs),
        scratch_shapes=list(scratch),
    )(*args)


def pairs(count, step, chosen):
    both = []
    for i in range(count):
        if chosen(i):
            both += [(i, (i + step) % count), ((i + step) % count, i)]
    return both


def swap(x, axis, step, chosen):
    return lax.ppermute(x, axis, pairs(lax.axis_size(axis), step, chosen))


def even(i):
    return i % 2 == 0


def odd(i):
    return i % 2 == 1


def gather_all(block):
    ring = lax.all_to_all(block, Z_RING, 0, 0)
    copies = jnp.broadcast_to(ring[None], (32, *ring.shape))
    return lax.all_to_all(copies, PLANE, 0, 0)


def x_window(d):
    first = lax.axis_index("gx_2") == 0
    partner = swap(d, GX, 1, even)
    chip = jnp.where(first, jnp.concatenate([d, partner]), jnp.concatenate([partner, d]))
    far = swap(jnp.where(first, chip[:24], chip[8:]), GX, 1, odd)
    near = swap(jnp.where(first, chip[24:], chip[:8]), GX, 3, even)
    return jnp.where(first, jnp.concatenate([far, chip, near]), jnp.concatenate([near, chip, far]))


def per_device(particle_cell, particle_mass):
    tile_x = lax.axis_index(GX)
    tile_y = lax.axis_index(GY)
    pos = jnp.stack([tile_x, tile_y]).astype(jnp.int32)
    cells = particle_cell.reshape(512, 128)
    masses = particle_mass.reshape(512, 128)
    density = call(deposit_kernel, f32(128, 128), (), cells, masses).reshape(CX, CY, NZ)
    wide = x_window(density)
    strips = (
        swap(wide, GY, 1, even),
        swap(wide, GY, 1, odd),
        swap(wide, GY, 2, lambda i: i % 4 < 2),
        swap(wide, GY, 2, lambda i: i % 4 >= 2),
        swap(wide, GY, 3, even),
        swap(wide, GY, 3, odd),
    )
    send, d, u0, b1, u1 = call(
        pre_kernel, (f32(16, 2, NZ), f32(W0X, W0Y, NZ), *LEVELS_OUT), (vmem(64, NZ),), wide, *strips, pos=pos
    )
    got = gather_all(send).reshape(512, 2, NZ)
    send, u0, b1, u1, stat = call(
        mid_kernel,
        (f32(16, 2, NZ), *LEVELS_OUT, f32(16, NZ)),
        (vmem(W1X, W1Y, NZ), *COARSE_SCRATCH),
        got, d, u0, b1, u1,
        pos=pos,
    )
    got = gather_all(send).reshape(512, 2, NZ)
    potential, residual, sums = call(
        post_kernel,
        (f32(CX, CY, NZ), f32(CX, CY, NZ), f32(16, 1, NZ)),
        (vmem(W0X, W0Y, NZ), vmem(W1X, W1Y, NZ), *COARSE_SCRATCH),
        got, d, u0, b1, u1, stat,
        pos=pos,
    )
    ring = jnp.sum(lax.all_to_all(sums, Z_RING, 0, 0), axis=0)
    total = jnp.sum(lax.all_to_all(jnp.broadcast_to(ring[None], (32, 1, NZ)), PLANE, 0, 0), axis=(0, 1))
    norms = jnp.sqrt(total[:2] / GRID_CELLS + norm_eps)
    return potential, residual, norms


def solution(mesh):
    split = Mesh(mesh.devices.reshape(2, 4, 2, 8, 4), ("gx_0", "gx_1", "gx_2", "gy_0", "gy_1"))
    placed = (P(GX, GY, None), P(GX, GY, None))
    return jax.shard_map(
        per_device,
        mesh=split,
        in_specs=placed,
        out_specs=(P(GX, GY, None), P(GX, GY, None), P()),
        check_vma=False,
    )
```

```python
import functools

import jax
import jax.numpy as jnp
from jax import lax
from jax.experimental import pallas as pl
from jax.experimental.pallas import tpu as pltpu
from jax.sharding import Mesh
from jax.sharding import PartitionSpec as P

CX = 16
CY = 8
NZ = 128
GX = ("gx_0", "gx_1", "gx_2")
GY = ("gy_0", "gy_1")
Z_RING = ("gx_0", "gy_0")
PLANE = ("gx_1", "gx_2", "gy_1")
TILES_X = 16
TILES_Y = 32
GRID_CELLS = 256 * 256 * 128
COARSE_CELLS = 64 * 64 * 32

coupling = 0.03125
norm_eps = 1e-06

W0X, W0Y = 64, 56
W1X, W1Y = 32, 32
W2X, W2Y = 36, 40
W3X, W3Y = 18, 24
DEPOSIT_ROWS = 32
KEEP = True
VMEM = pltpu.VMEM


def deposit_kernel(cell_ref, mass_ref, out_ref):
    rows = lax.broadcasted_iota(jnp.int32, (128, 128), 0)
    batch = DEPOSIT_ROWS

    def step(t, acc):
        cells = cell_ref[pl.ds(pl.multiple_of(t * batch, 8), batch), :]
        masses = mass_ref[pl.ds(pl.multiple_of(t * batch, 8), batch), :]
        high = cells >> 7
        low = cells & 127
        coarse = masses.astype(jnp.bfloat16).astype(jnp.float32)
        fine = masses - coarse
        left, right = [], []
        for r in range(batch):
            hit = rows == high[r : r + 1, :]
            first = jnp.where(hit, coarse[r : r + 1, :], 0.0).astype(jnp.bfloat16)
            second = jnp.where(hit, fine[r : r + 1, :], 0.0).astype(jnp.bfloat16)
            left.append(jnp.concatenate([first, second], axis=0))
            right.append(jnp.where(rows == low[r : r + 1, :], 1.0, 0.0).astype(jnp.bfloat16))
        left = jnp.concatenate(left, axis=1)
        right = jnp.concatenate(right, axis=1)
        return acc + lax.dot_general(left, right, (((1,), (1,)), ((), ())), preferred_element_type=jnp.float32)

    total = lax.fori_loop(0, cell_ref.shape[0] // batch, step, jnp.zeros((256, 128), jnp.float32))
    out_ref[...] = total[:128] + total[128:]


def row_parity(rows, lanes_per_cell, extra=0):
    j = lax.broadcasted_iota(jnp.int32, (rows, NZ), 0)
    z = lax.broadcasted_iota(jnp.int32, (rows, NZ), 1) // lanes_per_cell
    return (j + z + extra) & 1


def around(ref, i, rows, lanes, top=0):
    part = slice(top, top + rows)
    c = ref[i, part, :]
    n = ref[i - 1, part, :] + ref[i + 1, part, :]
    n = n + (pltpu.roll(c, 1, 0) + pltpu.roll(c, rows - 1, 0))
    return c, n + (pltpu.roll(c, lanes, 1) + pltpu.roll(c, NZ - lanes, 1))


def pair_z(t, lanes):
    z = lax.broadcasted_iota(jnp.int32, t.shape, 1) // lanes
    return t + jnp.where((z & 1) == 0, pltpu.roll(t, NZ - lanes, 1), pltpu.roll(t, lanes, 1))


def loop(lo, hi, body, unroll=2):
    def step(i, carry):
        body(i)
        return carry

    lax.fori_loop(lo, hi, step, 0, unroll=unroll)


def first_sweep(u, b, parity, rows, lanes, s, lo, hi):
    def body(i):
        c, n = around(b, i, rows, lanes)
        red = parity == (i & 1)
        u[i] = jnp.where(red, c * (s / 6.0), n * (s / 36.0) + c * (s / 6.0))

    loop(lo, hi, body)


def half_sweep(u, get_b, parity, colour, rows, lanes, s, lo, hi, top=0):
    def body(i):
        c, n = around(u, i, rows, lanes, top)
        chosen = parity == ((i + colour) & 1)
        u[i, top : top + rows, :] = jnp.where(chosen, (n + s * get_b(i)) * (1.0 / 6.0), c)

    loop(lo, hi, body)


def residual_at(u, b, i, rows, lanes, s, top=0):
    c, n = around(u, i, rows, lanes, top)
    return b - (6.0 * c - n) * (1.0 / s)


def restrict_to(out, u, get_b, rows, lanes, s, lo, hi, scr, out_rows, top=0):
    def body(p):
        t = residual_at(u, get_b(2 * p), 2 * p, rows, lanes, s, top)
        t = t + residual_at(u, get_b(2 * p + 1), 2 * p + 1, rows, lanes, s, top)
        scr[top : top + rows, :] = pair_z(t, lanes)
        out[p] = (scr[pl.ds(0, out_rows, 2), :] + scr[pl.ds(1, out_rows, 2), :]) * 0.125

    loop(lo, hi, body, 1)


def spread_rows(value, rows, scr):
    scr[pl.ds(0, rows, 2), :] = value
    scr[pl.ds(1, rows, 2), :] = value
    return scr[0 : 2 * rows, :]


def own_coarse(u1, b1, send_ref):
    lane = lax.broadcasted_iota(jnp.int32, (W1Y, NZ), 1) & 3
    packed = jnp.zeros((W1Y, NZ), jnp.float32)
    for x in range(4):
        i = 12 + 2 * x
        t = residual_at(u1, b1[i], i, W1Y, 2, 4.0) + residual_at(u1, b1[i + 1], i + 1, W1Y, 2, 4.0)
        t = pair_z(t, 2)
        t = (t + pltpu.roll(t, W1Y - 1, 0)) * 0.125
        packed = jnp.where(lane == x, t, packed)
    for k in range(send_ref.shape[0]):
        send_ref[k, 0:1, :] = packed[12:13, :]
        send_ref[k, 1:2, :] = packed[14:15, :]


def coarse_solve(pos_ref, ag, shift, pw, b2, u2, b3, u3, scr):
    gx, gy = pos_ref[0], pos_ref[1]
    pw[...] = jnp.zeros(pw.shape, jnp.float32)
    for tx in range(9):
        x = lax.rem(gx + (tx - 4 + TILES_X), TILES_X)
        for ty in range(17):
            y = lax.rem(gy + (ty - 8 + TILES_Y), TILES_Y)
            plane = (x & 7) * 4 + (y & 3)
            ring = (x >> 3) * 8 + (y >> 2)
            pw[tx, 2 * ty : 2 * ty + 2, :] = ag[plane * 16 + ring]
    lane = lax.broadcasted_iota(jnp.int32, (W2Y, NZ), 1) & 3

    def unpack(tx):
        t = pw[tx]
        for j in range(4):
            v = jnp.where(lane == j, t, 0.0)
            v = v + pltpu.roll(v, 1 if j % 2 == 0 else NZ - 1, 1)
            v = v + pltpu.roll(v, 2 if j < 2 else NZ - 2, 1)
            b2[4 * tx + j] = v - shift

    loop(0, 9, unpack, 1)
    par2 = row_parity(W2Y, 4)
    u2[0] = jnp.zeros((W2Y, NZ), jnp.float32)
    u2[W2X - 1] = jnp.zeros((W2Y, NZ), jnp.float32)
    first_sweep(u2, b2, par2, W2Y, 4, 16.0, 1, W2X - 1)
    scr[32:64, :] = jnp.zeros((32, NZ), jnp.float32)
    for i in (0, W3X - 1):
        b3[i] = jnp.zeros((W3Y, NZ), jnp.float32)
        u3[i] = jnp.zeros((W3Y, NZ), jnp.float32)
    restrict_to(b3, u2, lambda i: b2[i], W2Y, 4, 16.0, 1, W3X - 1, scr, W3Y)
    par3 = row_parity(W3Y, 8, gy)
    first_sweep(u3, b3, par3, W3Y, 8, 64.0, 1, W3X - 1)
    for colour in (0, 1):
        half_sweep(u3, lambda i: b3[i], par3, colour, W3Y, 8, 64.0, 1, W3X - 1)

    def add(p):
        c = spread_rows(u3[p], W3Y, scr)[0:W2Y]
        u2[2 * p] = u2[2 * p] + c
        u2[2 * p + 1] = u2[2 * p + 1] + c

    loop(4, 14, add, 1)
    half_sweep(u2, lambda i: b2[i], par2, 0, W2Y, 4, 16.0, 9, 27)
    half_sweep(u2, lambda i: b2[i], par2, 1, W2Y, 4, 16.0, 10, 26)


def up_level1(v1, u1, b1, shift, u2, scr, lo, hi, top, rows):
    part = slice(top, top + rows)
    first = 10 + top // 2

    def add(p):
        c = spread_rows(u2[p + 10, first : first + rows // 2, :], rows // 2, scr)
        v1[2 * p, part, :] = u1[2 * p, part, :] - shift * (4.0 / 3.0) + c
        v1[2 * p + 1, part, :] = u1[2 * p + 1, part, :] - shift * (4.0 / 3.0) + c

    loop(lo // 2, hi // 2, add, 1)
    par1 = row_parity(rows, 2)
    for colour in (0, 1):
        half_sweep(v1, lambda i: b1[i, part, :] - shift, par1, colour, rows, 2, 4.0, lo + 1, hi - 1, top)


def up_level0(v0, u0, d, shift, base, v1, scr, lo, hi, top, rows):
    part = slice(top, top + rows)
    half = (rows // 2 + 7) // 8 * 8

    def add(p):
        c = spread_rows(v1[p, top // 2 : top // 2 + half, :], half, scr)[0:rows]
        v0[2 * p, part, :] = u0[2 * p, part, :] - base + c
        v0[2 * p + 1, part, :] = u0[2 * p + 1, part, :] - base + c

    loop(lo // 2, hi // 2, add, 1)
    par0 = row_parity(rows, 1)
    for colour in (0, 1):
        half_sweep(v0, lambda i: d[i, part, :] - shift, par0, colour, rows, 1, 1.0, lo + 1, hi - 1, top)


def down_level1(u1, b1, send_ref):
    u1[0] = jnp.zeros((W1Y, NZ), jnp.float32)
    u1[W1X - 1] = jnp.zeros((W1Y, NZ), jnp.float32)
    first_sweep(u1, b1, row_parity(W1Y, 2), W1Y, 2, 4.0, 1, W1X - 1)
    own_coarse(u1, b1, send_ref)


def pre_kernel(pos_ref, x_ref, p1e, p1o, p2a, p2b, p3a, p3b, send_ref, d, u0, b1, u1, scr):
    gy = pos_ref[1]
    d[:, 24:32, :] = x_ref[...]

    def place(first, second, offset):
        d[:, 24 + offset : 32 + offset, :] = first[...]
        d[:, 24 - offset : 32 - offset, :] = second[...]

    even = (gy & 1) == 0
    low = (gy & 3) < 2
    for cond, a, b, offset in ((even, p1e, p1o, 8), (low, p2a, p2b, 16), (even, p3a, p3b, 24)):
        pl.when(cond)(functools.partial(place, a, b, offset))
        pl.when(jnp.logical_not(cond))(functools.partial(place, b, a, offset))
    for i in (0, W0X - 1):
        u0[i] = jnp.zeros((W0Y, NZ), jnp.float32)
    first_sweep(u0, d, row_parity(W0Y, 1), W0Y, 1, 1.0, 1, W0X - 1)
    scr[...] = jnp.zeros(scr.shape, jnp.float32)
    for i in (0, W1X - 1):
        b1[i] = jnp.zeros((W1Y, NZ), jnp.float32)
    restrict_to(b1, u0, lambda i: d[i], W0Y, 1, 1.0, 1, W1X - 1, scr, W1Y)
    down_level1(u1, b1, send_ref)


def own_residual(u, d, shift, x):
    i = 24 + x
    return residual_at(u, d[i, 16:40, :] - shift, i, 24, 1, 1.0, 16)[8:16]


def mid_kernel(pos_ref, ag, d, u0, b1, u1, send_ref, u0n, b1n, u1n, stat_ref, v1, pw, b2, u2, b3, u3, scr):
    total = jnp.sum(jnp.sum(ag[...], axis=0))
    mean = total * (1.0 / COARSE_CELLS)
    coarse_solve(pos_ref, ag, mean, pw, b2, u2, b3, u3, scr)
    up_level1(v1, u1, b1, mean, u2, scr, 0, W1X, 0, W1Y)
    up_level0(u0n, u0, d, mean, mean * (1.0 / 3.0), v1, scr, 8, 56, 8, 40)
    squares = jnp.zeros((CY, NZ), jnp.float32)
    for x in range(CX):
        r = own_residual(u0n, d, mean, x)
        squares = squares + r * r
    stat_ref[0:8, :] = squares
    stat_ref[8:16, :] = jnp.full((8, NZ), mean, jnp.float32)
    par0 = row_parity(40, 1)
    for colour in (0, 1):
        half_sweep(u0n, lambda i: d[i, 8:48, :] - mean, par0, colour, 40, 1, 1.0, 10, 54, 8)
    scr[...] = jnp.zeros(scr.shape, jnp.float32)
    for i in range(W1X):
        if i < 6 or i >= 26:
            b1n[i] = jnp.zeros((W1Y, NZ), jnp.float32)
    restrict_to(b1n, u0n, lambda i: d[i, 8:48, :] - mean, 40, 1, 1.0, 6, 26, scr, W1Y, 8)
    down_level1(u1n, b1n, send_ref)


def post_kernel(pos_ref, ag, d, u0, b1, u1, stat, pot_ref, res_ref, sums_ref, v0, v1, pw, b2, u2, b3, u3, scr):
    mean = jnp.max(stat[8:16, :])
    coarse_solve(pos_ref, ag, 0.0, pw, b2, u2, b3, u3, scr)
    up_level1(v1, u1, b1, 0.0, u2, scr, 8, 24, 8, 16)
    up_level0(v0, u0, d, mean, 0.0, v1, scr, 20, 44, 16, 24)
    inv = 1.0 / jnp.full((CY, NZ), mean, jnp.float32)
    total = jnp.zeros((CY, NZ), jnp.float32)
    for i in range(CX):
        r = own_residual(v0, d, mean, i) * inv
        total = total + r * r
        res_ref[i] = -r
        pot_ref[i] = v0[24 + i, 24:32, :] * (-coupling * inv)
    first = stat[0:8, :] * (inv * inv)
    lane = lax.broadcasted_iota(jnp.int32, (1, NZ), 1)
    both = jnp.where(lane == 0, jnp.sum(first), 0.0) + jnp.where(lane == 1, jnp.sum(total), 0.0)
    for k in range(sums_ref.shape[0]):
        sums_ref[k] = both


def f32(*shape):
    return jax.ShapeDtypeStruct(shape, jnp.float32)


def kept(*shape):
    return pltpu.VMEM(shape, jnp.float32) if KEEP else f32(*shape)


def resident(x):
    return pltpu.with_memory_space_constraint(x, pltpu.VMEM) if KEEP else x


def vmem(*shape):
    return pltpu.VMEM(shape, jnp.float32)


COARSE_SCRATCH = (vmem(9, W2Y, NZ), vmem(W2X, W2Y, NZ), vmem(W2X, W2Y, NZ), vmem(W3X, W3Y, NZ), vmem(W3X, W3Y, NZ), vmem(64, NZ))
LEVELS_OUT = (kept(W0X, W0Y, NZ), kept(W1X, W1Y, NZ), kept(W1X, W1Y, NZ))


def call(kernel, outs, scratch, *args, pos=None):
    whole = pl.BlockSpec(memory_space=VMEM)
    specs = [whole] * len(args)
    args = tuple(resident(a) for a in args)
    if pos is not None:
        specs = [pl.BlockSpec(memory_space=pltpu.SMEM)] + specs
        args = (pos, *args)
    return pl.pallas_call(
        kernel,
        out_shape=outs,
        in_specs=specs,
        out_specs=jax.tree.map(lambda _: whole, outs),
        scratch_shapes=list(scratch),
        compiler_params=pltpu.CompilerParams(vmem_limit_bytes=24 * 1024 * 1024),
    )(*args)


def pairs(count, step, chosen):
    both = []
    for i in range(count):
        if chosen(i):
            both += [(i, (i + step) % count), ((i + step) % count, i)]
    return both


def swap(x, axis, step, chosen):
    return lax.ppermute(x, axis, pairs(lax.axis_size(axis), step, chosen))


def even(i):
    return i % 2 == 0


def odd(i):
    return i % 2 == 1


def gather_all(block):
    ring = lax.all_to_all(block, Z_RING, 0, 0)
    copies = jnp.broadcast_to(ring[None], (32, *ring.shape))
    return lax.all_to_all(copies, PLANE, 0, 0)


def x_window(d):
    first = lax.axis_index("gx_2") == 0
    partner = swap(d, GX, 1, even)
    chip = jnp.where(first, jnp.concatenate([d, partner]), jnp.concatenate([partner, d]))
    far = swap(jnp.where(first, chip[:24], chip[8:]), GX, 1, odd)
    near = swap(jnp.where(first, chip[24:], chip[:8]), GX, 3, even)
    return jnp.where(first, jnp.concatenate([far, chip, near]), jnp.concatenate([near, chip, far]))


def per_device(particle_cell, particle_mass):
    tile_x = lax.axis_index(GX)
    tile_y = lax.axis_index(GY)
    pos = jnp.stack([tile_x, tile_y]).astype(jnp.int32)
    cells = particle_cell.reshape(512, 128)
    masses = particle_mass.reshape(512, 128)
    density = call(deposit_kernel, kept(128, 128), (), cells, masses).reshape(CX, CY, NZ)
    wide = x_window(density)
    strips = (
        swap(wide, GY, 1, even),
        swap(wide, GY, 1, odd),
        swap(wide, GY, 2, lambda i: i % 4 < 2),
        swap(wide, GY, 2, lambda i: i % 4 >= 2),
        swap(wide, GY, 3, even),
        swap(wide, GY, 3, odd),
    )
    send, d, u0, b1, u1 = call(
        pre_kernel, (kept(16, 2, NZ), kept(W0X, W0Y, NZ), *LEVELS_OUT), (vmem(64, NZ),), wide, *strips, pos=pos
    )
    got = gather_all(send).reshape(512, 2, NZ)
    send, u0, b1, u1, stat = call(
        mid_kernel,
        (kept(16, 2, NZ), *LEVELS_OUT, kept(16, NZ)),
        (vmem(W1X, W1Y, NZ), *COARSE_SCRATCH),
        got, d, u0, b1, u1,
        pos=pos,
    )
    got = gather_all(send).reshape(512, 2, NZ)
    potential, residual, sums = call(
        post_kernel,
        (f32(CX, CY, NZ), f32(CX, CY, NZ), kept(16, 1, NZ)),
        (vmem(W0X, W0Y, NZ), vmem(W1X, W1Y, NZ), *COARSE_SCRATCH),
        got, d, u0, b1, u1, stat,
        pos=pos,
    )
    ring = jnp.sum(lax.all_to_all(sums, Z_RING, 0, 0), axis=0)
    total = jnp.sum(lax.all_to_all(jnp.broadcast_to(ring[None], (32, 1, NZ)), PLANE, 0, 0), axis=(0, 1))
    norms = jnp.sqrt(total[:2] / GRID_CELLS + norm_eps)
    return potential, residual, norms


def solution(mesh):
    split = Mesh(mesh.devices.reshape(2, 4, 2, 8, 4), ("gx_0", "gx_1", "gx_2", "gy_0", "gy_1"))
    placed = (P(GX, GY, None), P(GX, GY, None))
    return jax.shard_map(
        per_device,
        mesh=split,
        in_specs=placed,
        out_specs=(P(GX, GY, None), P(GX, GY, None), P()),
        check_vma=False,
    )
```

```python
import functools

import jax
import jax.numpy as jnp
from jax import lax
from jax.experimental import pallas as pl
from jax.experimental.pallas import tpu as pltpu
from jax.sharding import Mesh
from jax.sharding import PartitionSpec as P

CX = 16
CY = 8
NZ = 128
GX = ("gx_0", "gx_1", "gx_2")
GY = ("gy_0", "gy_1")
Z_RING = ("gx_0", "gy_0")
PLANE = ("gx_1", "gx_2", "gy_1")
TILES_X = 16
TILES_Y = 32
GRID_CELLS = 256 * 256 * 128
COARSE_CELLS = 64 * 64 * 32

coupling = 0.03125
norm_eps = 1e-06

W0X, W0Y = 64, 56
W1X, W1Y = 32, 32
W2X, W2Y = 36, 40
W3X, W3Y = 18, 24
DEPOSIT_ROWS = 32
KEEP = True
VMEM = pltpu.VMEM


def deposit_kernel(cell_ref, mass_ref, out_ref):
    rows = lax.broadcasted_iota(jnp.int32, (128, 128), 0)
    batch = DEPOSIT_ROWS

    def step(t, acc):
        cells = cell_ref[pl.ds(pl.multiple_of(t * batch, 8), batch), :]
        masses = mass_ref[pl.ds(pl.multiple_of(t * batch, 8), batch), :]
        high = cells >> 7
        low = cells & 127
        coarse = masses.astype(jnp.bfloat16).astype(jnp.float32)
        fine = masses - coarse
        left, right = [], []
        for r in range(batch):
            hit = rows == high[r : r + 1, :]
            first = jnp.where(hit, coarse[r : r + 1, :], 0.0).astype(jnp.bfloat16)
            second = jnp.where(hit, fine[r : r + 1, :], 0.0).astype(jnp.bfloat16)
            left.append(jnp.concatenate([first, second], axis=0))
            right.append(jnp.where(rows == low[r : r + 1, :], 1.0, 0.0).astype(jnp.bfloat16))
        left = jnp.concatenate(left, axis=1)
        right = jnp.concatenate(right, axis=1)
        return acc + lax.dot_general(left, right, (((1,), (1,)), ((), ())), preferred_element_type=jnp.float32)

    total = lax.fori_loop(0, cell_ref.shape[0] // batch, step, jnp.zeros((256, 128), jnp.float32))
    out_ref[...] = total[:128] + total[128:]


def row_parity(rows, lanes_per_cell, extra=0):
    j = lax.broadcasted_iota(jnp.int32, (rows, NZ), 0)
    z = lax.broadcasted_iota(jnp.int32, (rows, NZ), 1) // lanes_per_cell
    return (j + z + extra) & 1


def batched(lo, hi, size, body):
    whole = (hi - lo) // size

    def step(t, carry):
        body(lo + t * size, size)
        return carry

    if whole:
        lax.fori_loop(0, whole, step, 0)
    if (hi - lo) % size:
        body(lo + whole * size, (hi - lo) % size)


def batch_of(rows):
    return 4 if rows >= 40 else 6 if rows >= 24 else 8


def planes(ref, first, count, part):
    return [ref[first + j, part, :] for j in range(count)]


def neighbours(values, j, lanes):
    c = values[j]
    rows = c.shape[0]
    n = values[j - 1] + values[j + 1]
    n = n + (pltpu.roll(c, 1, 0) + pltpu.roll(c, rows - 1, 0))
    return c, n + (pltpu.roll(c, lanes, 1) + pltpu.roll(c, NZ - lanes, 1))


def pair_z(t, lanes):
    z = lax.broadcasted_iota(jnp.int32, t.shape, 1) // lanes
    return t + jnp.where((z & 1) == 0, pltpu.roll(t, NZ - lanes, 1), pltpu.roll(t, lanes, 1))


def first_sweep(u, b, parity, lanes, s, lo, hi):
    rows = parity.shape[0]
    red = (parity == 0, parity == 1)

    def body(first, count):
        values = planes(b, first - 1, count + 2, slice(0, rows))
        for j in range(count):
            c, n = neighbours(values, j + 1, lanes)
            own = c * (s / 6.0)
            u[first + j, 0:rows, :] = jnp.where(red[(lo + j) & 1], own, n * (s / 36.0) + own)

    batched(lo, hi, batch_of(rows), body)


def half_sweep(u, b, shift, parity, colour, lanes, s, lo, hi, top=0):
    rows = parity.shape[0]
    part = slice(top, top + rows)
    chosen = (parity == (colour & 1), parity == ((1 + colour) & 1))

    def body(first, count):
        values = planes(u, first - 1, count + 2, part)
        made = []
        for j in range(count):
            c, n = neighbours(values, j + 1, lanes)
            rhs = (b[first + j, part, :] - shift) * (s / 6.0)
            made.append(jnp.where(chosen[(lo + j) & 1], n * (1.0 / 6.0) + rhs, c))
        for j in range(count):
            u[first + j, part, :] = made[j]

    batched(lo, hi, batch_of(rows), body)


def residual_of(values, j, b, lanes, s):
    c, n = neighbours(values, j, lanes)
    return b - (6.0 * c - n) * (1.0 / s)


def restrict_to(out, u, b, shift, rows, lanes, s, lo, hi, scr, out_rows, top=0):
    part = slice(top, top + rows)

    def body(first, count):
        values = planes(u, 2 * first - 1, 2 * count + 2, part)
        for k in range(count):
            t = residual_of(values, 2 * k + 1, b[2 * (first + k), part, :] - shift, lanes, s)
            t = t + residual_of(values, 2 * k + 2, b[2 * (first + k) + 1, part, :] - shift, lanes, s)
            scr[k, part, :] = pair_z(t, lanes)
        for k in range(count):
            out[first + k] = (scr.at[k][pl.ds(0, out_rows, 2), :] + scr.at[k][pl.ds(1, out_rows, 2), :]) * 0.125

    batched(lo, hi, 2, body)


def add_coarse(fine, base, shift, coarse, offset, first_row, half, lo, hi, top, rows, scr):
    part = slice(top, top + rows)

    def body(first, count):
        for k in range(count):
            c = coarse[first + k + offset, first_row : first_row + half, :]
            scr.at[k][pl.ds(0, half, 2), :] = c
            scr.at[k][pl.ds(1, half, 2), :] = c
        for k in range(count):
            c = scr[k, 0:rows, :] - shift
            i = 2 * (first + k)
            even, odd = base[i, part, :] + c, base[i + 1, part, :] + c
            fine[i, part, :] = even
            fine[i + 1, part, :] = odd

    batched(lo, hi, 4, body)


def own_coarse(u1, b1, send_ref, rows, plane, row):
    lane = lax.broadcasted_iota(jnp.int32, (rows, NZ), 1) & 3
    packed = jnp.zeros((rows, NZ), jnp.float32)
    values = planes(u1, plane - 1, 10, slice(0, rows))
    for x in range(4):
        i = plane + 2 * x
        t = residual_of(values, 2 * x + 1, b1[i, 0:rows, :], 2, 4.0)
        t = t + residual_of(values, 2 * x + 2, b1[i + 1, 0:rows, :], 2, 4.0)
        t = pair_z(t, 2)
        t = (t + pltpu.roll(t, rows - 1, 0)) * 0.125
        packed = jnp.where(lane == x, t, packed)
    for k in range(send_ref.shape[0]):
        send_ref[k, 0:1, :] = packed[row : row + 1, :]
        send_ref[k, 1:2, :] = packed[row + 2 : row + 3, :]


def clear(ref, *indices):
    for i in indices:
        ref[i] = jnp.zeros(ref.shape[1:], jnp.float32)


def coarse_solve(pos_ref, ag, shift, pw, b2, u2, b3, u3, scr):
    gx, gy = pos_ref[0], pos_ref[1]
    for tx in range(9):
        pw[tx, 32:40, :] = jnp.zeros((8, NZ), jnp.float32)
        x = lax.rem(gx + (tx - 4 + TILES_X), TILES_X)
        for ty in range(17):
            y = lax.rem(gy + (ty - 8 + TILES_Y), TILES_Y)
            plane = (x & 7) * 4 + (y & 3)
            ring = (x >> 3) * 8 + (y >> 2)
            pw[tx, 2 * ty : 2 * ty + 2, :] = ag[plane * 16 + ring]
    lane = lax.broadcasted_iota(jnp.int32, (W2Y, NZ), 1) & 3

    def unpack(tx, count):
        t = pw[tx]
        for j in range(4):
            v = jnp.where(lane == j, t, 0.0)
            v = v + pltpu.roll(v, 1 if j % 2 == 0 else NZ - 1, 1)
            v = v + pltpu.roll(v, 2 if j < 2 else NZ - 2, 1)
            b2[4 * tx + j] = v - shift

    batched(0, 9, 1, unpack)
    par2 = row_parity(W2Y, 4)
    clear(u2, 0, W2X - 1)
    first_sweep(u2, b2, par2, 4, 16.0, 1, W2X - 1)
    clear(scr, 0, 1)
    clear(b3, 0, W3X - 1)
    clear(u3, 0, W3X - 1)
    restrict_to(b3, u2, b2, 0.0, W2Y, 4, 16.0, 1, W3X - 1, scr, W3Y)
    par3 = row_parity(W3Y, 8, gy)
    first_sweep(u3, b3, par3, 8, 64.0, 1, W3X - 1)
    for colour in (0, 1):
        half_sweep(u3, b3, 0.0, par3, colour, 8, 64.0, 2, W3X - 2)
    add_coarse(u2, u2, 0.0, u3, 0, 0, W3Y, 4, 14, 0, W2Y, scr)
    half_sweep(u2, b2, 0.0, par2, 0, 4, 16.0, 9, 27)
    half_sweep(u2, b2, 0.0, par2, 1, 4, 16.0, 10, 26)


def up_level1(v1, u1, b1, shift, u2, scr, lo, hi, top, rows):
    add_coarse(v1, u1, shift * (4.0 / 3.0), u2, 10, 10 + top // 2, rows // 2, lo // 2, hi // 2, top, rows, scr)
    par1 = row_parity(rows, 2)
    for colour in (0, 1):
        half_sweep(v1, b1, shift, par1, colour, 2, 4.0, lo + 1, hi - 1, top)


def up_level0(v0, u0, d, shift, base, v1, scr, lo, hi, top, rows):
    half = (rows // 2 + 7) // 8 * 8
    add_coarse(v0, u0, base, v1, 0, top // 2, half, lo // 2, hi // 2, top, rows, scr)
    par0 = row_parity(rows, 1)
    for colour in (0, 1):
        half_sweep(v0, d, shift, par0, colour, 1, 1.0, lo + 1, hi - 1, top)


def join_rows(d, pos_ref, wide, e, o, first, last, own):
    d[:, own : own + 8, :] = wide[first:last]
    even = (pos_ref[1] & 1) == 0

    def place(e_row, o_row):
        d[:, e_row : e_row + 8, :] = e[first:last]
        d[:, o_row : o_row + 8, :] = o[first:last]

    pl.when(even)(functools.partial(place, own + 8, own - 8))
    pl.when(jnp.logical_not(even))(functools.partial(place, own - 8, own + 8))


def send_kernel(pos_ref, wide, e, o, send_ref, d, u0, b1, u1, scr):
    join_rows(d, pos_ref, wide, e, o, 16, 48, 8)
    clear(u0, 0, 31)
    first_sweep(u0, d, row_parity(24, 1), 1, 1.0, 1, 31)
    clear(scr, 0, 1)
    clear(b1, 0, 15)
    clear(u1, 0, 15)
    restrict_to(b1, u0, d, 0.0, 24, 1, 1.0, 1, 15, scr, 16)
    first_sweep(u1, b1, row_parity(16, 2), 2, 4.0, 1, 15)
    own_coarse(u1, b1, send_ref, 16, 4, 4)


def own_residual(u, d, shift):
    values = planes(u, 23, 18, slice(16, 40))
    return [residual_of(values, x + 1, d[24 + x, 16:40, :] - shift, 1, 1.0)[8:16] for x in range(CX)]


def wide_kernel(pos_ref, wide, e, o, s, t, d, u0, b1, u1, scr):
    for i in range(16):
        d[i] = jnp.zeros((W0Y, NZ), jnp.float32)
        d[48 + i] = jnp.zeros((W0Y, NZ), jnp.float32)
    join_rows(d, pos_ref, wide, e, o, 0, 64, 24)
    even = (pos_ref[1] & 1) == 0

    def place(o_row, s_row, s_far, t_row):
        d[8:56, o_row : o_row + 8, :] = o[64:112]
        d[8:56, s_row : s_row + 8, :] = s[0:48]
        d[16:48, s_far : s_far + 8, :] = s[48:80]
        d[16:48, t_row : t_row + 8, :] = t[...]

    pl.when(even)(functools.partial(place, 8, 40, 48, 0))
    pl.when(jnp.logical_not(even))(functools.partial(place, 40, 8, 0, 48))
    clear(u0, 0, W0X - 1)
    first_sweep(u0, d, row_parity(W0Y, 1), 1, 1.0, 1, W0X - 1)
    clear(scr, 0, 1)
    clear(b1, 0, W1X - 1)
    clear(u1, 0, W1X - 1)
    restrict_to(b1, u0, d, 0.0, W0Y, 1, 1.0, 1, W1X - 1, scr, W1Y)
    first_sweep(u1, b1, row_parity(W1Y, 2), 2, 4.0, 1, W1X - 1)


def mid_kernel(pos_ref, ag, d, u0, b1, u1, send_ref, u0n, b1n, u1n, stat_ref, v1, pw, b2, u2, b3, u3, scr):
    total = jnp.sum(jnp.sum(ag[...], axis=0))
    mean = total * (1.0 / COARSE_CELLS)
    clear(scr, 2, 3)
    coarse_solve(pos_ref, ag, mean, pw, b2, u2, b3, u3, scr)
    up_level1(v1, u1, b1, mean, u2, scr, 0, W1X, 0, W1Y)
    up_level0(u0n, u0, d, mean, mean * (1.0 / 3.0), v1, scr, 8, 56, 8, 40)
    stat_ref[0:8, :] = sum(r * r for r in own_residual(u0n, d, mean))
    stat_ref[8:16, :] = jnp.full((8, NZ), mean, jnp.float32)
    par0 = row_parity(40, 1)
    for colour in (0, 1):
        half_sweep(u0n, d, mean, par0, colour, 1, 1.0, 10, 54, 8)
    clear(scr, 0, 1)
    clear(b1n, *range(6), *range(26, W1X))
    restrict_to(b1n, u0n, d, mean, 40, 1, 1.0, 6, 26, scr, W1Y, 8)
    clear(u1n, 0, W1X - 1)
    first_sweep(u1n, b1n, row_parity(W1Y, 2), 2, 4.0, 1, W1X - 1)
    own_coarse(u1n, b1n, send_ref, W1Y, 12, 12)


def post_kernel(pos_ref, ag, d, u0, b1, u1, stat, pot_ref, res_ref, sums_ref, v0, v1, pw, b2, u2, b3, u3, scr):
    mean = jnp.max(stat[8:16, :])
    coarse_solve(pos_ref, ag, 0.0, pw, b2, u2, b3, u3, scr)
    up_level1(v1, u1, b1, 0.0, u2, scr, 8, 24, 8, 16)
    up_level0(v0, u0, d, mean, 0.0, v1, scr, 20, 44, 16, 24)
    inv = 1.0 / jnp.full((CY, NZ), mean, jnp.float32)
    total = jnp.zeros((CY, NZ), jnp.float32)
    for i, r in enumerate(own_residual(v0, d, mean)):
        r = r * inv
        total = total + r * r
        res_ref[i] = -r
        pot_ref[i] = v0[24 + i, 24:32, :] * (-coupling * inv)
    first = stat[0:8, :] * (inv * inv)
    lane = lax.broadcasted_iota(jnp.int32, (1, NZ), 1)
    both = jnp.where(lane == 0, jnp.sum(first), 0.0) + jnp.where(lane == 1, jnp.sum(total), 0.0)
    for k in range(sums_ref.shape[0]):
        sums_ref[k] = both


def f32(*shape):
    return jax.ShapeDtypeStruct(shape, jnp.float32)


def kept(*shape):
    return pltpu.VMEM(shape, jnp.float32) if KEEP else f32(*shape)


def resident(x):
    return pltpu.with_memory_space_constraint(x, pltpu.VMEM) if KEEP else x


def vmem(*shape):
    return pltpu.VMEM(shape, jnp.float32)


COARSE_SCRATCH = (vmem(9, W2Y, NZ), vmem(W2X, W2Y, NZ), vmem(W2X, W2Y, NZ), vmem(W3X, W3Y, NZ), vmem(W3X, W3Y, NZ), vmem(4, 64, NZ))
LEVELS_OUT = (kept(W0X, W0Y, NZ), kept(W1X, W1Y, NZ), kept(W1X, W1Y, NZ))


def call(kernel, outs, scratch, *args, pos=None, cost=None):
    whole = pl.BlockSpec(memory_space=VMEM)
    specs = [whole] * len(args)
    args = tuple(resident(a) for a in args)
    if pos is not None:
        specs = [pl.BlockSpec(memory_space=pltpu.SMEM)] + specs
        args = (pos, *args)
    return pl.pallas_call(
        kernel,
        out_shape=outs,
        in_specs=specs,
        out_specs=jax.tree.map(lambda _: whole, outs),
        scratch_shapes=list(scratch),
        cost_estimate=cost and pl.CostEstimate(flops=cost, transcendentals=0, bytes_accessed=0),
        compiler_params=pltpu.CompilerParams(vmem_limit_bytes=24 * 1024 * 1024),
    )(*args)


def pairs(count, step, chosen):
    both = []
    for i in range(count):
        if chosen(i):
            both += [(i, (i + step) % count), ((i + step) % count, i)]
    return both


def swap(x, axis, step, chosen):
    return lax.ppermute(x, axis, pairs(lax.axis_size(axis), step, chosen))


def even(i):
    return i % 2 == 0


def odd(i):
    return i % 2 == 1


def gather_all(block):
    ring = lax.all_to_all(block, Z_RING, 0, 0)
    copies = jnp.broadcast_to(ring[None], (32, *ring.shape))
    return lax.all_to_all(copies, PLANE, 0, 0)


def x_window(d):
    first = lax.axis_index("gx_2") == 0
    partner = swap(d, GX, 1, even)
    chip = jnp.where(first, jnp.concatenate([d, partner]), jnp.concatenate([partner, d]))
    far = swap(jnp.where(first, chip[:24], chip[8:]), GX, 1, odd)
    near = swap(jnp.where(first, chip[24:], chip[:8]), GX, 3, even)
    return jnp.where(first, jnp.concatenate([far, chip, near]), jnp.concatenate([near, chip, far]))


def per_device(particle_cell, particle_mass):
    tile_x = lax.axis_index(GX)
    tile_y = lax.axis_index(GY)
    pos = jnp.stack([tile_x, tile_y]).astype(jnp.int32)
    cells = particle_cell.reshape(512, 128)
    masses = particle_mass.reshape(512, 128)
    density = call(deposit_kernel, kept(128, 128), (), cells, masses).reshape(CX, CY, NZ)
    wide = x_window(density)
    e = swap(wide, GY, 1, even)
    t = swap(wide[16:48], GY, 3, odd)
    o = swap(jnp.concatenate([wide, e[8:56]]), GY, 1, odd)
    s = swap(jnp.concatenate([e[8:56], wide[16:48]]), GY, 3, even)
    send = call(
        send_kernel,
        kept(16, 2, NZ),
        (vmem(32, 24, NZ), vmem(32, 24, NZ), vmem(16, 16, NZ), vmem(16, 16, NZ), vmem(4, 64, NZ)),
        wide, e, o,
        pos=pos,
    )
    got = gather_all(send).reshape(512, 2, NZ)
    d, u0, b1, u1 = call(
        wide_kernel, (kept(W0X, W0Y, NZ), *LEVELS_OUT), (vmem(4, 64, NZ),), wide, e, o, s, t, pos=pos, cost=20_000_000
    )
    send, u0, b1, u1, stat = call(
        mid_kernel,
        (kept(16, 2, NZ), *LEVELS_OUT, kept(16, NZ)),
        (vmem(W1X, W1Y, NZ), *COARSE_SCRATCH),
        got, d, u0, b1, u1,
        pos=pos,
    )
    got = gather_all(send).reshape(512, 2, NZ)
    potential, residual, sums = call(
        post_kernel,
        (f32(CX, CY, NZ), f32(CX, CY, NZ), kept(16, 1, NZ)),
        (vmem(W0X, W0Y, NZ), vmem(W1X, W1Y, NZ), *COARSE_SCRATCH),
        got, d, u0, b1, u1, stat,
        pos=pos,
    )
    ring = jnp.sum(lax.all_to_all(sums, Z_RING, 0, 0), axis=0)
    total = jnp.sum(lax.all_to_all(jnp.broadcast_to(ring[None], (32, 1, NZ)), PLANE, 0, 0), axis=(0, 1))
    norms = jnp.sqrt(total[:2] / GRID_CELLS + norm_eps)
    return potential, residual, norms


def solution(mesh):
    split = Mesh(mesh.devices.reshape(2, 4, 2, 8, 4), ("gx_0", "gx_1", "gx_2", "gy_0", "gy_1"))
    placed = (P(GX, GY, None), P(GX, GY, None))
    return jax.shard_map(
        per_device,
        mesh=split,
        in_specs=placed,
        out_specs=(P(GX, GY, None), P(GX, GY, None), P()),
        check_vma=False,
    )
```

```python
import functools

import jax
import jax.numpy as jnp
from jax import lax
from jax.experimental import pallas as pl
from jax.experimental.pallas import tpu as pltpu
from jax.sharding import Mesh
from jax.sharding import PartitionSpec as P

CX = 16
CY = 8
NZ = 128
GX = ("gx_0", "gx_1", "gx_2")
GY = ("gy_0", "gy_1")
Z_RING = ("gx_0", "gy_0")
PLANE = ("gx_1", "gx_2", "gy_1")
TILES_X = 16
TILES_Y = 32
GRID_CELLS = 256 * 256 * 128
COARSE_CELLS = 64 * 64 * 32

coupling = 0.03125
norm_eps = 1e-06

W0X, W0Y = 64, 56
W1X, W1Y = 32, 32
W2X, W2Y = 36, 40
W3X, W3Y = 18, 24
DEPOSIT_ROWS = 32
KEEP = True
RESTRICT = 4
ADD = 4
SIZES = (6, 8, 10, 16, 16)
VMEM = pltpu.VMEM


def deposit_kernel(cell_ref, mass_ref, out_ref):
    rows = lax.broadcasted_iota(jnp.int32, (128, 128), 0)
    batch = DEPOSIT_ROWS

    def step(t, acc):
        cells = cell_ref[pl.ds(pl.multiple_of(t * batch, 8), batch), :]
        masses = mass_ref[pl.ds(pl.multiple_of(t * batch, 8), batch), :]
        high = cells >> 7
        low = cells & 127
        coarse = masses.astype(jnp.bfloat16).astype(jnp.float32)
        fine = masses - coarse
        left, right = [], []
        for r in range(batch):
            hit = rows == high[r : r + 1, :]
            first = jnp.where(hit, coarse[r : r + 1, :], 0.0).astype(jnp.bfloat16)
            second = jnp.where(hit, fine[r : r + 1, :], 0.0).astype(jnp.bfloat16)
            left.append(jnp.concatenate([first, second], axis=0))
            right.append(jnp.where(rows == low[r : r + 1, :], 1.0, 0.0).astype(jnp.bfloat16))
        left = jnp.concatenate(left, axis=1)
        right = jnp.concatenate(right, axis=1)
        return acc + lax.dot_general(left, right, (((1,), (1,)), ((), ())), preferred_element_type=jnp.float32)

    total = lax.fori_loop(0, cell_ref.shape[0] // batch, step, jnp.zeros((256, 128), jnp.float32))
    out_ref[...] = total[:128] + total[128:]


def row_parity(rows, lanes_per_cell, extra=0):
    j = lax.broadcasted_iota(jnp.int32, (rows, NZ), 0)
    z = lax.broadcasted_iota(jnp.int32, (rows, NZ), 1) // lanes_per_cell
    return (j + z + extra) & 1


def batched(lo, hi, size, body):
    size = min(size, hi - lo)
    runs = -(-(hi - lo) // size)
    if runs == 1:
        body(lo, size)
        return

    def step(t, carry):
        body(jnp.minimum(lo + t * size, hi - size), size)
        return carry

    lax.fori_loop(0, runs, step, 0)


def batch_of(rows):
    return {56: SIZES[0], 40: SIZES[1], 32: SIZES[2], 24: SIZES[3], 16: SIZES[4]}[rows]


def planes(ref, first, count, part):
    return [ref[first + j, part, :] for j in range(count)]


def neighbours(values, j, lanes):
    c = values[j]
    rows = c.shape[0]
    n = values[j - 1] + values[j + 1]
    n = n + (pltpu.roll(c, 1, 0) + pltpu.roll(c, rows - 1, 0))
    return c, n + (pltpu.roll(c, lanes, 1) + pltpu.roll(c, NZ - lanes, 1))


def pair_z(t, lanes):
    z = lax.broadcasted_iota(jnp.int32, t.shape, 1) // lanes
    return t + jnp.where((z & 1) == 0, pltpu.roll(t, NZ - lanes, 1), pltpu.roll(t, lanes, 1))


def first_sweep(u, b, parity, lanes, s, lo, hi):
    rows = parity.shape[0]
    red = (parity == 0, parity == 1)

    def body(first, count):
        values = planes(b, first - 1, count + 2, slice(0, rows))
        for j in range(count):
            c, n = neighbours(values, j + 1, lanes)
            own = c * (s / 6.0)
            u[first + j, 0:rows, :] = jnp.where(red[(lo + j) & 1], own, n * (s / 36.0) + own)

    batched(lo, hi, batch_of(rows), body)


def half_sweep(u, b, shift, parity, colour, lanes, s, lo, hi, top=0):
    rows = parity.shape[0]
    part = slice(top, top + rows)
    chosen = (parity == (colour & 1), parity == ((1 + colour) & 1))

    def body(first, count):
        values = planes(u, first - 1, count + 2, part)
        made = []
        for j in range(count):
            c, n = neighbours(values, j + 1, lanes)
            rhs = (b[first + j, part, :] - shift) * (s / 6.0)
            made.append(jnp.where(chosen[(lo + j) & 1], n * (1.0 / 6.0) + rhs, c))
        for j in range(count):
            u[first + j, part, :] = made[j]

    batched(lo, hi, batch_of(rows), body)


def residual_of(values, j, b, lanes, s):
    c, n = neighbours(values, j, lanes)
    return b - (6.0 * c - n) * (1.0 / s)


def restrict_to(out, u, b, shift, rows, lanes, s, lo, hi, scr, out_rows, top=0):
    part = slice(top, top + rows)

    def body(first, count):
        values = planes(u, 2 * first - 1, 2 * count + 2, part)
        for k in range(count):
            t = residual_of(values, 2 * k + 1, b[2 * (first + k), part, :] - shift, lanes, s)
            t = t + residual_of(values, 2 * k + 2, b[2 * (first + k) + 1, part, :] - shift, lanes, s)
            scr[k, part, :] = pair_z(t, lanes)
        for k in range(count):
            out[first + k] = (scr.at[k][pl.ds(0, out_rows, 2), :] + scr.at[k][pl.ds(1, out_rows, 2), :]) * 0.125

    batched(lo, hi, RESTRICT, body)


def add_coarse(fine, base, shift, coarse, offset, first_row, half, lo, hi, top, rows, scr):
    part = slice(top, top + rows)

    def body(first, count):
        for k in range(count):
            c = coarse[first + k + offset, first_row : first_row + half, :]
            scr.at[k][pl.ds(0, half, 2), :] = c
            scr.at[k][pl.ds(1, half, 2), :] = c
        for k in range(count):
            c = scr[k, 0:rows, :] - shift
            i = 2 * (first + k)
            even, odd = base[i, part, :] + c, base[i + 1, part, :] + c
            fine[i, part, :] = even
            fine[i + 1, part, :] = odd

    batched(lo, hi, (hi - lo) // 2 if base is fine else ADD, body)


def own_coarse(u1, b1, send_ref, rows, plane, row):
    lane = lax.broadcasted_iota(jnp.int32, (rows, NZ), 1) & 3
    packed = jnp.zeros((rows, NZ), jnp.float32)
    values = planes(u1, plane - 1, 10, slice(0, rows))
    for x in range(4):
        i = plane + 2 * x
        t = residual_of(values, 2 * x + 1, b1[i, 0:rows, :], 2, 4.0)
        t = t + residual_of(values, 2 * x + 2, b1[i + 1, 0:rows, :], 2, 4.0)
        t = pair_z(t, 2)
        t = (t + pltpu.roll(t, rows - 1, 0)) * 0.125
        packed = jnp.where(lane == x, t, packed)
    for k in range(send_ref.shape[0]):
        send_ref[k, 0:1, :] = packed[row : row + 1, :]
        send_ref[k, 1:2, :] = packed[row + 2 : row + 3, :]


def clear(ref, *indices):
    for i in indices:
        ref[i] = jnp.zeros(ref.shape[1:], jnp.float32)


def coarse_solve(pos_ref, ag, shift, pw, b2, u2, b3, u3, scr):
    gx, gy = pos_ref[0], pos_ref[1]
    for tx in range(9):
        pw[tx, 32:40, :] = jnp.zeros((8, NZ), jnp.float32)
        x = lax.rem(gx + (tx - 4 + TILES_X), TILES_X)
        for ty in range(17):
            y = lax.rem(gy + (ty - 8 + TILES_Y), TILES_Y)
            plane = (x & 7) * 4 + (y & 3)
            ring = (x >> 3) * 8 + (y >> 2)
            pw[tx, 2 * ty : 2 * ty + 2, :] = ag[plane * 16 + ring]
    lane = lax.broadcasted_iota(jnp.int32, (W2Y, NZ), 1) & 3

    def unpack(first, count):
        for k in range(count):
            t = pw[first + k]
            for j in range(4):
                v = jnp.where(lane == j, t, 0.0)
                v = v + pltpu.roll(v, 1 if j % 2 == 0 else NZ - 1, 1)
                v = v + pltpu.roll(v, 2 if j < 2 else NZ - 2, 1)
                b2[4 * (first + k) + j] = v - shift

    batched(0, 9, 3, unpack)
    par2 = row_parity(W2Y, 4)
    clear(u2, 0, W2X - 1)
    first_sweep(u2, b2, par2, 4, 16.0, 1, W2X - 1)
    clear(scr, *range(RESTRICT))
    clear(b3, 0, W3X - 1)
    clear(u3, 0, W3X - 1)
    restrict_to(b3, u2, b2, 0.0, W2Y, 4, 16.0, 1, W3X - 1, scr, W3Y)
    par3 = row_parity(W3Y, 8, gy)
    first_sweep(u3, b3, par3, 8, 64.0, 1, W3X - 1)
    for colour in (0, 1):
        half_sweep(u3, b3, 0.0, par3, colour, 8, 64.0, 2, W3X - 2)
    add_coarse(u2, u2, 0.0, u3, 0, 0, W3Y, 4, 14, 0, W2Y, scr)
    half_sweep(u2, b2, 0.0, par2, 0, 4, 16.0, 9, 27)
    half_sweep(u2, b2, 0.0, par2, 1, 4, 16.0, 10, 26)


def up_level1(v1, u1, b1, shift, u2, scr, lo, hi, top, rows):
    add_coarse(v1, u1, shift * (4.0 / 3.0), u2, 10, 10 + top // 2, rows // 2, lo // 2, hi // 2, top, rows, scr)
    par1 = row_parity(rows, 2)
    for colour in (0, 1):
        half_sweep(v1, b1, shift, par1, colour, 2, 4.0, lo + 1, hi - 1, top)


def up_level0(v0, u0, d, shift, base, v1, scr, lo, hi, top, rows):
    half = (rows // 2 + 7) // 8 * 8
    add_coarse(v0, u0, base, v1, 0, top // 2, half, lo // 2, hi // 2, top, rows, scr)
    par0 = row_parity(rows, 1)
    for colour in (0, 1):
        half_sweep(v0, d, shift, par0, colour, 1, 1.0, lo + 1, hi - 1, top)


def beside(pos_ref, place, own):
    even = (pos_ref[1] & 1) == 0
    pl.when(even)(functools.partial(place, own + 8, own - 8))
    pl.when(jnp.logical_not(even))(functools.partial(place, own - 8, own + 8))


def send_kernel(pos_ref, wide, e, near, send_ref, d, u0, b1, u1, scr):
    d[:, 8:16, :] = wide[16:48]

    def place(e_row, o_row):
        d[:, e_row : e_row + 8, :] = e[16:48]
        d[:, o_row : o_row + 8, :] = near[...]

    beside(pos_ref, place, 8)
    clear(u0, 0, 31)
    first_sweep(u0, d, row_parity(24, 1), 1, 1.0, 1, 31)
    clear(scr, *range(RESTRICT))
    clear(b1, 0, 15)
    clear(u1, 0, 15)
    restrict_to(b1, u0, d, 0.0, 24, 1, 1.0, 1, 15, scr, 16)
    first_sweep(u1, b1, row_parity(16, 2), 2, 4.0, 1, 15)
    own_coarse(u1, b1, send_ref, 16, 4, 4)


def own_residual(u, d, shift):
    values = planes(u, 23, 18, slice(16, 40))
    return [residual_of(values, x + 1, d[24 + x, 16:40, :] - shift, 1, 1.0)[8:16] for x in range(CX)]


def mid_kernel(pos_ref, ag, wide, e, near, o, s, t, send_ref, d, u0n, b1n, u1n, stat_ref, u0, b1, u1, v1, pw, b2, u2, b3, u3, scr):
    total = jnp.sum(jnp.sum(ag[...], axis=0))
    mean = total * (1.0 / COARSE_CELLS)
    for i in range(16):
        d[i] = jnp.zeros((W0Y, NZ), jnp.float32)
        d[48 + i] = jnp.zeros((W0Y, NZ), jnp.float32)
    d[:, 24:32, :] = wide[...]

    def place_first(e_row, o_row):
        d[:, e_row : e_row + 8, :] = e[...]
        d[0:16, o_row : o_row + 8, :] = o[0:16]
        d[16:48, o_row : o_row + 8, :] = near[...]
        d[48:64, o_row : o_row + 8, :] = o[16:32]

    def place_second(s_row, o_row):
        d[8:56, s_row : s_row + 8, :] = s[0:48]
        d[8:56, o_row : o_row + 8, :] = o[32:80]

    def place_third(s_row, t_row):
        d[16:48, s_row : s_row + 8, :] = s[48:80]
        d[16:48, t_row : t_row + 8, :] = t[...]

    even = (pos_ref[1] & 1) == 0
    for offset, place in ((8, place_first), (16, place_second), (24, place_third)):
        pl.when(even)(functools.partial(place, 24 + offset, 24 - offset))
        pl.when(jnp.logical_not(even))(functools.partial(place, 24 - offset, 24 + offset))
    clear(u0, 0, W0X - 1)
    first_sweep(u0, d, row_parity(W0Y, 1), 1, 1.0, 1, W0X - 1)
    clear(scr, *range(8))
    clear(b1, 0, W1X - 1)
    clear(u1, 0, W1X - 1)
    restrict_to(b1, u0, d, 0.0, W0Y, 1, 1.0, 1, W1X - 1, scr, W1Y)
    first_sweep(u1, b1, row_parity(W1Y, 2), 2, 4.0, 1, W1X - 1)
    coarse_solve(pos_ref, ag, mean, pw, b2, u2, b3, u3, scr)
    up_level1(v1, u1, b1, mean, u2, scr, 0, W1X, 0, W1Y)
    up_level0(u0n, u0, d, mean, mean * (1.0 / 3.0), v1, scr, 8, 56, 8, 40)
    stat_ref[0:8, :] = sum(r * r for r in own_residual(u0n, d, mean))
    stat_ref[8:16, :] = jnp.full((8, NZ), mean, jnp.float32)
    par0 = row_parity(40, 1)
    for colour in (0, 1):
        half_sweep(u0n, d, mean, par0, colour, 1, 1.0, 10, 54, 8)
    clear(scr, *range(RESTRICT))
    clear(b1n, *range(6), *range(26, W1X))
    restrict_to(b1n, u0n, d, mean, 40, 1, 1.0, 6, 26, scr, W1Y, 8)
    clear(u1n, 0, W1X - 1)
    first_sweep(u1n, b1n, row_parity(W1Y, 2), 2, 4.0, 1, W1X - 1)
    own_coarse(u1n, b1n, send_ref, W1Y, 12, 12)


def post_kernel(pos_ref, ag, d, u0, b1, u1, stat, pot_ref, res_ref, sums_ref, v0, v1, pw, b2, u2, b3, u3, scr):
    mean = jnp.max(stat[8:16, :])
    coarse_solve(pos_ref, ag, 0.0, pw, b2, u2, b3, u3, scr)
    up_level1(v1, u1, b1, 0.0, u2, scr, 8, 24, 8, 16)
    up_level0(v0, u0, d, mean, 0.0, v1, scr, 20, 44, 16, 24)
    inv = 1.0 / jnp.full((CY, NZ), mean, jnp.float32)
    total = jnp.zeros((CY, NZ), jnp.float32)
    for i, r in enumerate(own_residual(v0, d, mean)):
        r = r * inv
        total = total + r * r
        res_ref[i] = -r
        pot_ref[i] = v0[24 + i, 24:32, :] * (-coupling * inv)
    first = stat[0:8, :] * (inv * inv)
    lane = lax.broadcasted_iota(jnp.int32, (1, NZ), 1)
    both = jnp.where(lane == 0, jnp.sum(first), 0.0) + jnp.where(lane == 1, jnp.sum(total), 0.0)
    for k in range(sums_ref.shape[0]):
        sums_ref[k] = both


def f32(*shape):
    return jax.ShapeDtypeStruct(shape, jnp.float32)


def kept(*shape):
    return pltpu.VMEM(shape, jnp.float32) if KEEP else f32(*shape)


def resident(x):
    return pltpu.with_memory_space_constraint(x, pltpu.VMEM) if KEEP else x


def vmem(*shape):
    return pltpu.VMEM(shape, jnp.float32)


COARSE_SCRATCH = (vmem(9, W2Y, NZ), vmem(W2X, W2Y, NZ), vmem(W2X, W2Y, NZ), vmem(W3X, W3Y, NZ), vmem(W3X, W3Y, NZ), vmem(8, 64, NZ))
LEVELS_OUT = (kept(W0X, W0Y, NZ), kept(W1X, W1Y, NZ), kept(W1X, W1Y, NZ))


def call(kernel, outs, scratch, *args, pos=None):
    whole = pl.BlockSpec(memory_space=VMEM)
    specs = [whole] * len(args)
    args = tuple(resident(a) for a in args)
    if pos is not None:
        specs = [pl.BlockSpec(memory_space=pltpu.SMEM)] + specs
        args = (pos, *args)
    return pl.pallas_call(
        kernel,
        out_shape=outs,
        in_specs=specs,
        out_specs=jax.tree.map(lambda _: whole, outs),
        scratch_shapes=list(scratch),
        compiler_params=pltpu.CompilerParams(vmem_limit_bytes=24 * 1024 * 1024),
    )(*args)


def pairs(count, step, chosen):
    both = []
    for i in range(count):
        if chosen(i):
            both += [(i, (i + step) % count), ((i + step) % count, i)]
    return both


def swap(x, axis, step, chosen):
    return lax.ppermute(x, axis, pairs(lax.axis_size(axis), step, chosen))


def even(i):
    return i % 2 == 0


def odd(i):
    return i % 2 == 1


def gather_all(block):
    ring = lax.all_to_all(block, Z_RING, 0, 0)
    copies = jnp.broadcast_to(ring[None], (32, *ring.shape))
    return lax.all_to_all(copies, PLANE, 0, 0)


def x_window(d):
    first = lax.axis_index("gx_2") == 0
    partner = swap(d, GX, 1, even)
    chip = jnp.where(first, jnp.concatenate([d, partner]), jnp.concatenate([partner, d]))
    far = swap(jnp.where(first, chip[:24], chip[8:]), GX, 1, odd)
    near = swap(jnp.where(first, chip[24:], chip[:8]), GX, 3, even)
    return jnp.where(first, jnp.concatenate([far, chip, near]), jnp.concatenate([near, chip, far]))


def per_device(particle_cell, particle_mass):
    tile_x = lax.axis_index(GX)
    tile_y = lax.axis_index(GY)
    pos = jnp.stack([tile_x, tile_y]).astype(jnp.int32)
    cells = particle_cell.reshape(512, 128)
    masses = particle_mass.reshape(512, 128)
    density = call(deposit_kernel, kept(128, 128), (), cells, masses).reshape(CX, CY, NZ)
    wide = x_window(density)
    e = swap(wide, GY, 1, even)
    near = swap(wide[16:48], GY, 1, odd)
    outer = jnp.concatenate([wide[:16], wide[48:], e[8:56]])
    reach = jnp.concatenate([e[8:56], wide[16:48]])
    send = call(
        send_kernel,
        kept(16, 2, NZ),
        (vmem(32, 24, NZ), vmem(32, 24, NZ), vmem(16, 16, NZ), vmem(16, 16, NZ), vmem(8, 64, NZ)),
        wide, e, near,
        pos=pos,
    )
    got = gather_all(send).reshape(512, 2, NZ)
    o = swap(outer, GY, 1, odd)
    s = swap(reach, GY, 3, even)
    t = swap(wide[16:48], GY, 3, odd)
    send, d, u0, b1, u1, stat = call(
        mid_kernel,
        (kept(16, 2, NZ), kept(W0X, W0Y, NZ), *LEVELS_OUT, kept(16, NZ)),
        (vmem(W0X, W0Y, NZ), vmem(W1X, W1Y, NZ), vmem(W1X, W1Y, NZ), vmem(W1X, W1Y, NZ), *COARSE_SCRATCH),
        got, wide, e, near, o, s, t,
        pos=pos,
    )
    got = gather_all(send).reshape(512, 2, NZ)
    potential, residual, sums = call(
        post_kernel,
        (f32(CX, CY, NZ), f32(CX, CY, NZ), kept(16, 1, NZ)),
        (vmem(W0X, W0Y, NZ), vmem(W1X, W1Y, NZ), *COARSE_SCRATCH),
        got, d, u0, b1, u1, stat,
        pos=pos,
    )
    ring = jnp.sum(lax.all_to_all(sums, Z_RING, 0, 0), axis=0)
    total = jnp.sum(lax.all_to_all(jnp.broadcast_to(ring[None], (32, 1, NZ)), PLANE, 0, 0), axis=(0, 1))
    norms = jnp.sqrt(total[:2] / GRID_CELLS + norm_eps)
    return potential, residual, norms


def solution(mesh):
    split = Mesh(mesh.devices.reshape(2, 4, 2, 8, 4), ("gx_0", "gx_1", "gx_2", "gy_0", "gy_1"))
    placed = (P(GX, GY, None), P(GX, GY, None))
    return jax.shard_map(
        per_device,
        mesh=split,
        in_specs=placed,
        out_specs=(P(GX, GY, None), P(GX, GY, None), P()),
        check_vma=False,
    )
```

```python
import functools

import jax
import jax.numpy as jnp
from jax import lax
from jax.experimental import pallas as pl
from jax.experimental.pallas import tpu as pltpu
from jax.sharding import Mesh
from jax.sharding import PartitionSpec as P

CX = 16
CY = 8
NZ = 128
GX = ("gx_0", "gx_1", "gx_2")
GY = ("gy_0", "gy_1")
Z_RING = ("gx_0", "gy_0")
PLANE = ("gx_1", "gx_2", "gy_1")
TILES_X = 16
TILES_Y = 32
GRID_CELLS = 256 * 256 * 128
COARSE_CELLS = 64 * 64 * 32

coupling = 0.03125
norm_eps = 1e-06

W0X, W0Y = 64, 56
W1X, W1Y = 32, 32
W2X, W2Y = 36, 40
W3X, W3Y = 18, 24
DEPOSIT_ROWS = 32
KEEP = True
RESTRICT = 4
ADD = 4
SIZES = (6, 8, 10, 16, 16)
VMEM = pltpu.VMEM


def deposit_kernel(cell_ref, mass_ref, out_ref):
    rows = lax.broadcasted_iota(jnp.int32, (128, 128), 0)
    batch = DEPOSIT_ROWS

    def step(t, acc):
        cells = cell_ref[pl.ds(pl.multiple_of(t * batch, 8), batch), :]
        masses = mass_ref[pl.ds(pl.multiple_of(t * batch, 8), batch), :]
        high = cells >> 7
        low = cells & 127
        coarse = masses.astype(jnp.bfloat16).astype(jnp.float32)
        fine = masses - coarse
        left, right = [], []
        for r in range(batch):
            hit = rows == high[r : r + 1, :]
            first = jnp.where(hit, coarse[r : r + 1, :], 0.0).astype(jnp.bfloat16)
            second = jnp.where(hit, fine[r : r + 1, :], 0.0).astype(jnp.bfloat16)
            left.append(jnp.concatenate([first, second], axis=0))
            right.append(jnp.where(rows == low[r : r + 1, :], 1.0, 0.0).astype(jnp.bfloat16))
        left = jnp.concatenate(left, axis=1)
        right = jnp.concatenate(right, axis=1)
        return acc + lax.dot_general(left, right, (((1,), (1,)), ((), ())), preferred_element_type=jnp.float32)

    total = lax.fori_loop(0, cell_ref.shape[0] // batch, step, jnp.zeros((256, 128), jnp.float32))
    out_ref[...] = total[:128] + total[128:]


def row_parity(rows, lanes_per_cell, extra=0):
    j = lax.broadcasted_iota(jnp.int32, (rows, NZ), 0)
    z = lax.broadcasted_iota(jnp.int32, (rows, NZ), 1) // lanes_per_cell
    return (j + z + extra) & 1


def batched(lo, hi, size, body):
    size = min(size, hi - lo)
    runs = -(-(hi - lo) // size)
    if runs == 1:
        body(lo, size)
        return

    def step(t, carry):
        body(jnp.minimum(lo + t * size, hi - size), size)
        return carry

    lax.fori_loop(0, runs, step, 0)


def batch_of(rows):
    return {56: SIZES[0], 40: SIZES[1], 32: SIZES[2], 24: SIZES[3], 16: SIZES[4]}[rows]


def planes(ref, first, count, part):
    return [ref[first + j, part, :] for j in range(count)]


def neighbours(values, j, lanes):
    c = values[j]
    rows = c.shape[0]
    n = values[j - 1] + values[j + 1]
    n = n + (pltpu.roll(c, 1, 0) + pltpu.roll(c, rows - 1, 0))
    return c, n + (pltpu.roll(c, lanes, 1) + pltpu.roll(c, NZ - lanes, 1))


def pair_z(t, lanes):
    z = lax.broadcasted_iota(jnp.int32, t.shape, 1) // lanes
    return t + jnp.where((z & 1) == 0, pltpu.roll(t, NZ - lanes, 1), pltpu.roll(t, lanes, 1))


def first_sweep(u, b, parity, lanes, s, lo, hi):
    rows = parity.shape[0]
    red = (parity == 0, parity == 1)

    def body(first, count):
        values = planes(b, first - 1, count + 2, slice(0, rows))
        for j in range(count):
            c, n = neighbours(values, j + 1, lanes)
            own = c * (s / 6.0)
            u[first + j, 0:rows, :] = jnp.where(red[(lo + j) & 1], own, n * (s / 36.0) + own)

    batched(lo, hi, batch_of(rows), body)


def half_sweep(u, b, shift, parity, colour, lanes, s, lo, hi, top=0):
    rows = parity.shape[0]
    part = slice(top, top + rows)
    chosen = (parity == (colour & 1), parity == ((1 + colour) & 1))

    def body(first, count):
        values = planes(u, first - 1, count + 2, part)
        made = []
        for j in range(count):
            c, n = neighbours(values, j + 1, lanes)
            rhs = (b[first + j, part, :] - shift) * (s / 6.0)
            made.append(jnp.where(chosen[(lo + j) & 1], n * (1.0 / 6.0) + rhs, c))
        for j in range(count):
            u[first + j, part, :] = made[j]

    batched(lo, hi, batch_of(rows), body)


def residual_of(values, j, b, lanes, s):
    c, n = neighbours(values, j, lanes)
    return b - (6.0 * c - n) * (1.0 / s)


def restrict_to(out, u, b, shift, rows, lanes, s, lo, hi, scr, out_rows, top=0):
    part = slice(top, top + rows)

    def body(first, count):
        values = planes(u, 2 * first - 1, 2 * count + 2, part)
        for k in range(count):
            t = residual_of(values, 2 * k + 1, b[2 * (first + k), part, :] - shift, lanes, s)
            t = t + residual_of(values, 2 * k + 2, b[2 * (first + k) + 1, part, :] - shift, lanes, s)
            scr[k, part, :] = pair_z(t, lanes)
        for k in range(count):
            out[first + k] = (scr.at[k][pl.ds(0, out_rows, 2), :] + scr.at[k][pl.ds(1, out_rows, 2), :]) * 0.125

    batched(lo, hi, RESTRICT, body)


def add_coarse(fine, base, shift, coarse, offset, first_row, half, lo, hi, top, rows, scr):
    part = slice(top, top + rows)

    def body(first, count):
        for k in range(count):
            c = coarse[first + k + offset, first_row : first_row + half, :]
            scr.at[k][pl.ds(0, half, 2), :] = c
            scr.at[k][pl.ds(1, half, 2), :] = c
        for k in range(count):
            c = scr[k, 0:rows, :] - shift
            i = 2 * (first + k)
            even, odd = base[i, part, :] + c, base[i + 1, part, :] + c
            fine[i, part, :] = even
            fine[i + 1, part, :] = odd

    batched(lo, hi, (hi - lo) // 2 if base is fine else ADD, body)


def own_coarse(u1, b1, send_ref, rows, plane, row):
    lane = lax.broadcasted_iota(jnp.int32, (rows, NZ), 1) & 3
    packed = jnp.zeros((rows, NZ), jnp.float32)
    values = planes(u1, plane - 1, 10, slice(0, rows))
    for x in range(4):
        i = plane + 2 * x
        t = residual_of(values, 2 * x + 1, b1[i, 0:rows, :], 2, 4.0)
        t = t + residual_of(values, 2 * x + 2, b1[i + 1, 0:rows, :], 2, 4.0)
        t = pair_z(t, 2)
        t = (t + pltpu.roll(t, rows - 1, 0)) * 0.125
        packed = jnp.where(lane == x, t, packed)
    for k in range(send_ref.shape[0]):
        send_ref[k, 0:1, :] = packed[row : row + 1, :]
        send_ref[k, 1:2, :] = packed[row + 2 : row + 3, :]


def clear(ref, *indices):
    for i in indices:
        ref[i] = jnp.zeros(ref.shape[1:], jnp.float32)


def coarse_solve(pos_ref, ag, shift, pw, b2, u2, b3, u3, scr):
    gx, gy = pos_ref[0], pos_ref[1]
    for tx in range(9):
        pw[tx, 32:40, :] = jnp.zeros((8, NZ), jnp.float32)
        x = lax.rem(gx + (tx - 4 + TILES_X), TILES_X)
        for ty in range(17):
            y = lax.rem(gy + (ty - 8 + TILES_Y), TILES_Y)
            plane = (x & 7) * 4 + (y & 3)
            ring = (y >> 2) * 2 + (x >> 3)
            pw[tx, 2 * ty : 2 * ty + 2, :] = ag[plane * 16 + ring]
    lane = lax.broadcasted_iota(jnp.int32, (W2Y, NZ), 1) & 3

    def unpack(first, count):
        for k in range(count):
            t = pw[first + k]
            for j in range(4):
                v = jnp.where(lane == j, t, 0.0)
                v = v + pltpu.roll(v, 1 if j % 2 == 0 else NZ - 1, 1)
                v = v + pltpu.roll(v, 2 if j < 2 else NZ - 2, 1)
                b2[4 * (first + k) + j] = v - shift

    batched(0, 9, 3, unpack)
    par2 = row_parity(W2Y, 4)
    clear(u2, 0, W2X - 1)
    first_sweep(u2, b2, par2, 4, 16.0, 1, W2X - 1)
    clear(scr, *range(RESTRICT))
    clear(b3, 0, W3X - 1)
    clear(u3, 0, W3X - 1)
    restrict_to(b3, u2, b2, 0.0, W2Y, 4, 16.0, 1, W3X - 1, scr, W3Y)
    par3 = row_parity(W3Y, 8, gy)
    first_sweep(u3, b3, par3, 8, 64.0, 1, W3X - 1)
    for colour in (0, 1):
        half_sweep(u3, b3, 0.0, par3, colour, 8, 64.0, 2, W3X - 2)
    add_coarse(u2, u2, 0.0, u3, 0, 0, W3Y, 4, 14, 0, W2Y, scr)
    half_sweep(u2, b2, 0.0, par2, 0, 4, 16.0, 9, 27)
    half_sweep(u2, b2, 0.0, par2, 1, 4, 16.0, 10, 26)


def up_level1(v1, u1, b1, shift, u2, scr, lo, hi, top, rows):
    add_coarse(v1, u1, shift * (4.0 / 3.0), u2, 10, 10 + top // 2, rows // 2, lo // 2, hi // 2, top, rows, scr)
    par1 = row_parity(rows, 2)
    for colour in (0, 1):
        half_sweep(v1, b1, shift, par1, colour, 2, 4.0, lo + 1, hi - 1, top)


def up_level0(v0, u0, d, shift, base, v1, scr, lo, hi, top, rows):
    half = (rows // 2 + 7) // 8 * 8
    add_coarse(v0, u0, base, v1, 0, top // 2, half, lo // 2, hi // 2, top, rows, scr)
    par0 = row_parity(rows, 1)
    for colour in (0, 1):
        half_sweep(v0, d, shift, par0, colour, 1, 1.0, lo + 1, hi - 1, top)


def beside(pos_ref, place, own):
    even = (pos_ref[1] & 1) == 0
    pl.when(even)(functools.partial(place, own + 8, own - 8))
    pl.when(jnp.logical_not(even))(functools.partial(place, own - 8, own + 8))


def send_kernel(pos_ref, wide, e, near, send_ref, d, u0, b1, u1, scr):
    d[:, 8:16, :] = wide[16:48]

    def place(e_row, o_row):
        d[:, e_row : e_row + 8, :] = e[16:48]
        d[:, o_row : o_row + 8, :] = near[...]

    beside(pos_ref, place, 8)
    clear(u0, 0, 31)
    first_sweep(u0, d, row_parity(24, 1), 1, 1.0, 1, 31)
    clear(scr, *range(RESTRICT))
    clear(b1, 0, 15)
    clear(u1, 0, 15)
    restrict_to(b1, u0, d, 0.0, 24, 1, 1.0, 1, 15, scr, 16)
    first_sweep(u1, b1, row_parity(16, 2), 2, 4.0, 1, 15)
    own_coarse(u1, b1, send_ref, 16, 4, 4)


def own_residual(u, d, shift):
    values = planes(u, 23, 18, slice(16, 40))
    return [residual_of(values, x + 1, d[24 + x, 16:40, :] - shift, 1, 1.0)[8:16] for x in range(CX)]


def mid_kernel(pos_ref, ag, wide, e, near, o, s, t, send_ref, d, u0n, b1n, u1n, stat_ref, u0, b1, u1, v1, pw, b2, u2, b3, u3, scr):
    total = jnp.sum(jnp.sum(ag[...], axis=0))
    mean = total * (1.0 / COARSE_CELLS)
    for i in range(16):
        d[i] = jnp.zeros((W0Y, NZ), jnp.float32)
        d[48 + i] = jnp.zeros((W0Y, NZ), jnp.float32)
    d[:, 24:32, :] = wide[...]

    def place_first(e_row, o_row):
        d[:, e_row : e_row + 8, :] = e[...]
        d[0:16, o_row : o_row + 8, :] = o[0:16]
        d[16:48, o_row : o_row + 8, :] = near[...]
        d[48:64, o_row : o_row + 8, :] = o[16:32]

    def place_second(s_row, o_row):
        d[8:56, s_row : s_row + 8, :] = s[0:48]
        d[8:56, o_row : o_row + 8, :] = o[32:80]

    def place_third(s_row, t_row):
        d[16:48, s_row : s_row + 8, :] = s[48:80]
        d[16:48, t_row : t_row + 8, :] = t[...]

    even = (pos_ref[1] & 1) == 0
    for offset, place in ((8, place_first), (16, place_second), (24, place_third)):
        pl.when(even)(functools.partial(place, 24 + offset, 24 - offset))
        pl.when(jnp.logical_not(even))(functools.partial(place, 24 - offset, 24 + offset))
    clear(u0, 0, W0X - 1)
    first_sweep(u0, d, row_parity(W0Y, 1), 1, 1.0, 1, W0X - 1)
    clear(scr, *range(8))
    clear(b1, 0, W1X - 1)
    clear(u1, 0, W1X - 1)
    restrict_to(b1, u0, d, 0.0, W0Y, 1, 1.0, 1, W1X - 1, scr, W1Y)
    first_sweep(u1, b1, row_parity(W1Y, 2), 2, 4.0, 1, W1X - 1)
    coarse_solve(pos_ref, ag, mean, pw, b2, u2, b3, u3, scr)
    up_level1(v1, u1, b1, mean, u2, scr, 0, W1X, 0, W1Y)
    up_level0(u0n, u0, d, mean, mean * (1.0 / 3.0), v1, scr, 8, 56, 8, 40)
    stat_ref[0:8, :] = sum(r * r for r in own_residual(u0n, d, mean))
    stat_ref[8:16, :] = jnp.full((8, NZ), mean, jnp.float32)
    par0 = row_parity(40, 1)
    for colour in (0, 1):
        half_sweep(u0n, d, mean, par0, colour, 1, 1.0, 10, 54, 8)
    clear(scr, *range(RESTRICT))
    clear(b1n, *range(6), *range(26, W1X))
    restrict_to(b1n, u0n, d, mean, 40, 1, 1.0, 6, 26, scr, W1Y, 8)
    clear(u1n, 0, W1X - 1)
    first_sweep(u1n, b1n, row_parity(W1Y, 2), 2, 4.0, 1, W1X - 1)
    own_coarse(u1n, b1n, send_ref, W1Y, 12, 12)


def post_kernel(pos_ref, ag, d, u0, b1, u1, stat, pot_ref, res_ref, sums_ref, v0, v1, pw, b2, u2, b3, u3, scr):
    mean = jnp.max(stat[8:16, :])
    coarse_solve(pos_ref, ag, 0.0, pw, b2, u2, b3, u3, scr)
    up_level1(v1, u1, b1, 0.0, u2, scr, 8, 24, 8, 16)
    up_level0(v0, u0, d, mean, 0.0, v1, scr, 20, 44, 16, 24)
    inv = 1.0 / jnp.full((CY, NZ), mean, jnp.float32)
    total = jnp.zeros((CY, NZ), jnp.float32)
    for i, r in enumerate(own_residual(v0, d, mean)):
        r = r * inv
        total = total + r * r
        res_ref[i] = -r
        pot_ref[i] = v0[24 + i, 24:32, :] * (-coupling * inv)
    first = stat[0:8, :] * (inv * inv)
    lane = lax.broadcasted_iota(jnp.int32, (1, NZ), 1)
    both = jnp.where(lane == 0, jnp.sum(first), 0.0) + jnp.where(lane == 1, jnp.sum(total), 0.0)
    for k in range(sums_ref.shape[0]):
        sums_ref[k] = both


def f32(*shape):
    return jax.ShapeDtypeStruct(shape, jnp.float32)


def kept(*shape):
    return pltpu.VMEM(shape, jnp.float32) if KEEP else f32(*shape)


def resident(x):
    return pltpu.with_memory_space_constraint(x, pltpu.VMEM) if KEEP else x


def vmem(*shape):
    return pltpu.VMEM(shape, jnp.float32)


COARSE_SCRATCH = (vmem(9, W2Y, NZ), vmem(W2X, W2Y, NZ), vmem(W2X, W2Y, NZ), vmem(W3X, W3Y, NZ), vmem(W3X, W3Y, NZ), vmem(8, 64, NZ))
LEVELS_OUT = (kept(W0X, W0Y, NZ), kept(W1X, W1Y, NZ), kept(W1X, W1Y, NZ))


def call(kernel, outs, scratch, *args, pos=None):
    whole = pl.BlockSpec(memory_space=VMEM)
    specs = [whole] * len(args)
    args = tuple(resident(a) for a in args)
    if pos is not None:
        specs = [pl.BlockSpec(memory_space=pltpu.SMEM)] + specs
        args = (pos, *args)
    return pl.pallas_call(
        kernel,
        out_shape=outs,
        in_specs=specs,
        out_specs=jax.tree.map(lambda _: whole, outs),
        scratch_shapes=list(scratch),
        compiler_params=pltpu.CompilerParams(vmem_limit_bytes=24 * 1024 * 1024),
    )(*args)


def place_of(tile_x, tile_y):
    z = (tile_y // 4) * 2 + tile_x // 8
    return (((z // 8) * 8 + tile_x % 8) * 8 + z % 8) * 4 + tile_y % 4


def every_tile():
    return [(i, j) for i in range(TILES_X) for j in range(TILES_Y)]


def move(x, forth):
    moves = [(i * TILES_Y + j, place_of(i, j)) for i, j in every_tile()]
    return lax.ppermute(x, GX + GY, moves if forth else [(b, a) for a, b in moves])


def swap(x, axis, step, chosen):
    both = []
    for i, j in every_tile():
        if chosen(i if axis is GX else j):
            other = ((i + step) % TILES_X, j) if axis is GX else (i, (j + step) % TILES_Y)
            a, b = place_of(i, j), place_of(*other)
            both += [(a, b), (b, a)]
    return lax.ppermute(x, GX + GY, both)


def even(i):
    return i % 2 == 0


def odd(i):
    return i % 2 == 1


def gather_all(block):
    ring = lax.all_to_all(block, Z_RING, 0, 0)
    copies = jnp.broadcast_to(ring[None], (32, *ring.shape))
    return lax.all_to_all(copies, PLANE, 0, 0)


def x_window(d):
    first = lax.axis_index("gx_2") == 0
    partner = swap(d, GX, 1, even)
    chip = jnp.where(first, jnp.concatenate([d, partner]), jnp.concatenate([partner, d]))
    far = swap(jnp.where(first, chip[:24], chip[8:]), GX, 1, odd)
    near = swap(jnp.where(first, chip[24:], chip[:8]), GX, 3, even)
    return jnp.where(first, jnp.concatenate([far, chip, near]), jnp.concatenate([near, chip, far]))


def per_device(particle_cell, particle_mass):
    z = lax.axis_index(Z_RING)
    tile_x = (z % 2) * 8 + lax.axis_index(("gx_1", "gx_2"))
    tile_y = (z // 2) * 4 + lax.axis_index("gy_1")
    pos = jnp.stack([tile_x, tile_y]).astype(jnp.int32)
    cells = particle_cell.reshape(512, 128)
    masses = particle_mass.reshape(512, 128)
    density = call(deposit_kernel, kept(128, 128), (), cells, masses).reshape(CX, CY, NZ)
    wide = x_window(move(density, True))
    e = swap(wide, GY, 1, even)
    near = swap(wide[16:48], GY, 1, odd)
    outer = jnp.concatenate([wide[:16], wide[48:], e[8:56]])
    reach = jnp.concatenate([e[8:56], wide[16:48]])
    send = call(
        send_kernel,
        kept(16, 2, NZ),
        (vmem(32, 24, NZ), vmem(32, 24, NZ), vmem(16, 16, NZ), vmem(16, 16, NZ), vmem(8, 64, NZ)),
        wide, e, near,
        pos=pos,
    )
    got = gather_all(send).reshape(512, 2, NZ)
    o = swap(outer, GY, 1, odd)
    s = swap(reach, GY, 3, even)
    t = swap(wide[16:48], GY, 3, odd)
    send, d, u0, b1, u1, stat = call(
        mid_kernel,
        (kept(16, 2, NZ), kept(W0X, W0Y, NZ), *LEVELS_OUT, kept(16, NZ)),
        (vmem(W0X, W0Y, NZ), vmem(W1X, W1Y, NZ), vmem(W1X, W1Y, NZ), vmem(W1X, W1Y, NZ), *COARSE_SCRATCH),
        got, wide, e, near, o, s, t,
        pos=pos,
    )
    got = gather_all(send).reshape(512, 2, NZ)
    potential, residual, sums = call(
        post_kernel,
        (f32(CX, CY, NZ), f32(CX, CY, NZ), kept(16, 1, NZ)),
        (vmem(W0X, W0Y, NZ), vmem(W1X, W1Y, NZ), *COARSE_SCRATCH),
        got, d, u0, b1, u1, stat,
        pos=pos,
    )
    ring = jnp.sum(lax.all_to_all(sums, Z_RING, 0, 0), axis=0)
    total = jnp.sum(lax.all_to_all(jnp.broadcast_to(ring[None], (32, 1, NZ)), PLANE, 0, 0), axis=(0, 1))
    norms = jnp.sqrt(total[:2] / GRID_CELLS + norm_eps)
    return move(potential, False), move(residual, False), norms


def solution(mesh):
    split = Mesh(mesh.devices.reshape(2, 4, 2, 8, 4), ("gx_0", "gx_1", "gx_2", "gy_0", "gy_1"))
    placed = (P(GX, GY, None), P(GX, GY, None))
    return jax.shard_map(
        per_device,
        mesh=split,
        in_specs=placed,
        out_specs=(P(GX, GY, None), P(GX, GY, None), P()),
        check_vma=False,
    )
```

```python
import functools

import jax
import jax.numpy as jnp
from jax import lax
from jax.experimental import pallas as pl
from jax.experimental.pallas import tpu as pltpu
from jax.sharding import Mesh
from jax.sharding import PartitionSpec as P

CX = 16
CY = 8
NZ = 128
GX = ("gx_0", "gx_1", "gx_2")
GY = ("gy_0", "gy_1")
Z_RING = ("gx_0", "gy_0")
PLANE = ("gx_1", "gx_2", "gy_1")
TILES_X = 16
TILES_Y = 32
GRID_CELLS = 256 * 256 * 128
COARSE_CELLS = 64 * 64 * 32

coupling = 0.03125
norm_eps = 1e-06

W0X, W0Y = 64, 56
W1X, W1Y = 32, 32
W2X, W2Y = 36, 40
W3X, W3Y = 18, 24
DEPOSIT_ROWS = 64
KEEP = True
RING = 10
RESTRICT = 4
ADD = 4
SIZES = (6, 8, 10, 16, 16)
VMEM = pltpu.VMEM


def deposit_kernel(cell_ref, mass_ref, out_ref):
    rows = lax.broadcasted_iota(jnp.int32, (128, 128), 0).astype(jnp.bfloat16)
    batch = DEPOSIT_ROWS

    def step(t, acc):
        cells = cell_ref[pl.ds(pl.multiple_of(t * batch, 8), batch), :]
        masses = mass_ref[pl.ds(pl.multiple_of(t * batch, 8), batch), :]
        high = (cells >> 7).astype(jnp.bfloat16)
        low = (cells & 127).astype(jnp.bfloat16)
        coarse = masses.astype(jnp.bfloat16)
        fine = (masses - coarse.astype(jnp.float32)).astype(jnp.bfloat16)
        zero = jnp.zeros((128, 128), jnp.bfloat16)
        one = jnp.ones((128, 128), jnp.bfloat16)
        left, right = [], []
        for r in range(batch):
            line = lambda x: jnp.broadcast_to(x[r : r + 1, :], (128, 128))
            hit = rows == line(high)
            left.append(jnp.concatenate([jnp.where(hit, line(coarse), zero), jnp.where(hit, line(fine), zero)], axis=0))
            right.append(jnp.where(rows == line(low), one, zero))
        left = jnp.concatenate(left, axis=1)
        right = jnp.concatenate(right, axis=1)
        return acc + lax.dot_general(left, right, (((1,), (1,)), ((), ())), preferred_element_type=jnp.float32)

    total = lax.fori_loop(0, cell_ref.shape[0] // batch, step, jnp.zeros((256, 128), jnp.float32))
    out_ref[...] = total[:128] + total[128:]


def row_parity(rows, lanes_per_cell, extra=0):
    j = lax.broadcasted_iota(jnp.int32, (rows, NZ), 0)
    z = lax.broadcasted_iota(jnp.int32, (rows, NZ), 1) // lanes_per_cell
    return (j + z + extra) & 1


def batched(lo, hi, size, body):
    size = min(size, hi - lo)
    runs = -(-(hi - lo) // size)
    if runs == 1:
        body(lo, size)
        return

    def step(t, carry):
        body(jnp.minimum(lo + t * size, hi - size), size)
        return carry

    lax.fori_loop(0, runs, step, 0)


def batch_of(rows):
    return {56: SIZES[0], 40: SIZES[1], 32: SIZES[2], 24: SIZES[3], 16: SIZES[4]}[rows]


def planes(ref, first, count, part):
    return [ref[first + j, part, :] for j in range(count)]


def neighbours(values, j, lanes):
    c = values[j]
    rows = c.shape[0]
    n = values[j - 1] + values[j + 1]
    n = n + (pltpu.roll(c, 1, 0) + pltpu.roll(c, rows - 1, 0))
    return c, n + (pltpu.roll(c, lanes, 1) + pltpu.roll(c, NZ - lanes, 1))


def pair_z(t, lanes):
    z = lax.broadcasted_iota(jnp.int32, t.shape, 1) // lanes
    return t + jnp.where((z & 1) == 0, pltpu.roll(t, NZ - lanes, 1), pltpu.roll(t, lanes, 1))


def first_sweep(u, b, parity, lanes, s, lo, hi):
    rows = parity.shape[0]
    red = (parity == 0, parity == 1)

    def body(first, count):
        values = planes(b, first - 1, count + 2, slice(0, rows))
        for j in range(count):
            c, n = neighbours(values, j + 1, lanes)
            own = c * (s / 6.0)
            u[first + j, 0:rows, :] = jnp.where(red[(lo + j) & 1], own, n * (s / 36.0) + own)

    batched(lo, hi, batch_of(rows), body)


def half_sweep(u, b, shift, parity, colour, lanes, s, lo, hi, top=0):
    rows = parity.shape[0]
    part = slice(top, top + rows)
    chosen = (parity == (colour & 1), parity == ((1 + colour) & 1))

    def body(first, count):
        values = planes(u, first - 1, count + 2, part)
        made = []
        for j in range(count):
            c, n = neighbours(values, j + 1, lanes)
            rhs = (b[first + j, part, :] - shift) * (s / 6.0)
            made.append(jnp.where(chosen[(lo + j) & 1], n * (1.0 / 6.0) + rhs, c))
        for j in range(count):
            u[first + j, part, :] = made[j]

    batched(lo, hi, batch_of(rows), body)


def residual_of(values, j, b, lanes, s):
    c, n = neighbours(values, j, lanes)
    return b - (6.0 * c - n) * (1.0 / s)


def restrict_to(out, u, b, shift, rows, lanes, s, lo, hi, scr, out_rows, top=0):
    part = slice(top, top + rows)

    def body(first, count):
        values = planes(u, 2 * first - 1, 2 * count + 2, part)
        for k in range(count):
            t = residual_of(values, 2 * k + 1, b[2 * (first + k), part, :] - shift, lanes, s)
            t = t + residual_of(values, 2 * k + 2, b[2 * (first + k) + 1, part, :] - shift, lanes, s)
            scr[k, part, :] = pair_z(t, lanes)
        for k in range(count):
            out[first + k] = (scr.at[k][pl.ds(0, out_rows, 2), :] + scr.at[k][pl.ds(1, out_rows, 2), :]) * 0.125

    batched(lo, hi, RESTRICT, body)


def add_coarse(fine, base, shift, coarse, offset, first_row, half, lo, hi, top, rows, scr):
    part = slice(top, top + rows)

    def body(first, count):
        for k in range(count):
            c = coarse[first + k + offset, first_row : first_row + half, :]
            scr.at[k][pl.ds(0, half, 2), :] = c
            scr.at[k][pl.ds(1, half, 2), :] = c
        for k in range(count):
            c = scr[k, 0:rows, :] - shift
            i = 2 * (first + k)
            even, odd = base[i, part, :] + c, base[i + 1, part, :] + c
            fine[i, part, :] = even
            fine[i + 1, part, :] = odd

    batched(lo, hi, (hi - lo) // 2 if base is fine else ADD, body)


def own_coarse(u1, b1, send_ref, rows, plane, row):
    lane = lax.broadcasted_iota(jnp.int32, (rows, NZ), 1) & 3
    packed = jnp.zeros((rows, NZ), jnp.float32)
    values = planes(u1, plane - 1, 10, slice(0, rows))
    for x in range(4):
        i = plane + 2 * x
        t = residual_of(values, 2 * x + 1, b1[i, 0:rows, :], 2, 4.0)
        t = t + residual_of(values, 2 * x + 2, b1[i + 1, 0:rows, :], 2, 4.0)
        t = pair_z(t, 2)
        t = (t + pltpu.roll(t, rows - 1, 0)) * 0.125
        packed = jnp.where(lane == x, t, packed)
    for k in range(send_ref.shape[0]):
        send_ref[k, 0:1, :] = packed[row : row + 1, :]
        send_ref[k, 1:2, :] = packed[row + 2 : row + 3, :]


def clear(ref, *indices):
    for i in indices:
        ref[i] = jnp.zeros(ref.shape[1:], jnp.float32)


def fan_kernel(pos_ref, ring, out):
    block = lax.shift_right_logical(pos_ref[1], 2)
    parts = [ring[8 * h + ((block + (j + 6)) & 7)] for h in range(2) for j in range(5)]
    parts.append(jnp.sum(ring[...], axis=0))
    for n in range(32):
        for j in range(RING + 1):
            out[n, j] = parts[j]


def coarse_solve(pos_ref, ag, shift, pw, b2, u2, b3, u3, scr):
    gx, gy = pos_ref[0], pos_ref[1]
    for tx in range(9):
        pw[tx, 32:40, :] = jnp.zeros((8, NZ), jnp.float32)
        x = lax.rem(gx + (tx - 4 + TILES_X), TILES_X)
        for ty in range(17):
            y = lax.rem(gy + (ty - 8 + TILES_Y), TILES_Y)
            plane = (x & 7) * 4 + (y & 3)
            ring = (x >> 3) * 5 + (((y >> 2) - (gy >> 2) + 2) & 7)
            pw[tx, 2 * ty : 2 * ty + 2, :] = ag[plane * (RING + 1) + ring]
    lane = lax.broadcasted_iota(jnp.int32, (W2Y, NZ), 1) & 3

    def unpack(first, count):
        for k in range(count):
            t = pw[first + k]
            for j in range(4):
                v = jnp.where(lane == j, t, 0.0)
                v = v + pltpu.roll(v, 1 if j % 2 == 0 else NZ - 1, 1)
                v = v + pltpu.roll(v, 2 if j < 2 else NZ - 2, 1)
                b2[4 * (first + k) + j] = v - shift

    batched(0, 9, 3, unpack)
    par2 = row_parity(W2Y, 4)
    clear(u2, 0, W2X - 1)
    first_sweep(u2, b2, par2, 4, 16.0, 1, W2X - 1)
    clear(scr, *range(RESTRICT))
    clear(b3, 0, W3X - 1)
    clear(u3, 0, W3X - 1)
    restrict_to(b3, u2, b2, 0.0, W2Y, 4, 16.0, 1, W3X - 1, scr, W3Y)
    par3 = row_parity(W3Y, 8, gy)
    first_sweep(u3, b3, par3, 8, 64.0, 1, W3X - 1)
    for colour in (0, 1):
        half_sweep(u3, b3, 0.0, par3, colour, 8, 64.0, 2, W3X - 2)
    add_coarse(u2, u2, 0.0, u3, 0, 0, W3Y, 4, 14, 0, W2Y, scr)
    half_sweep(u2, b2, 0.0, par2, 0, 4, 16.0, 9, 27)
    half_sweep(u2, b2, 0.0, par2, 1, 4, 16.0, 10, 26)


def up_level1(v1, u1, b1, shift, u2, scr, lo, hi, top, rows):
    add_coarse(v1, u1, shift * (4.0 / 3.0), u2, 10, 10 + top // 2, rows // 2, lo // 2, hi // 2, top, rows, scr)
    par1 = row_parity(rows, 2)
    for colour in (0, 1):
        half_sweep(v1, b1, shift, par1, colour, 2, 4.0, lo + 1, hi - 1, top)


def up_level0(v0, u0, d, shift, base, v1, scr, lo, hi, top, rows):
    half = (rows // 2 + 7) // 8 * 8
    add_coarse(v0, u0, base, v1, 0, top // 2, half, lo // 2, hi // 2, top, rows, scr)
    par0 = row_parity(rows, 1)
    for colour in (0, 1):
        half_sweep(v0, d, shift, par0, colour, 1, 1.0, lo + 1, hi - 1, top)


def beside(pos_ref, place, own):
    even = (pos_ref[1] & 1) == 0
    pl.when(even)(functools.partial(place, own + 8, own - 8))
    pl.when(jnp.logical_not(even))(functools.partial(place, own - 8, own + 8))


def send_kernel(pos_ref, wide, e, near, send_ref, d, u0, b1, u1, scr):
    d[:, 8:16, :] = wide[16:48]

    def place(e_row, o_row):
        d[:, e_row : e_row + 8, :] = e[16:48]
        d[:, o_row : o_row + 8, :] = near[...]

    beside(pos_ref, place, 8)
    clear(u0, 0, 31)
    first_sweep(u0, d, row_parity(24, 1), 1, 1.0, 1, 31)
    clear(scr, *range(RESTRICT))
    clear(b1, 0, 15)
    clear(u1, 0, 15)
    restrict_to(b1, u0, d, 0.0, 24, 1, 1.0, 1, 15, scr, 16)
    first_sweep(u1, b1, row_parity(16, 2), 2, 4.0, 1, 15)
    own_coarse(u1, b1, send_ref, 16, 4, 4)


def own_residual(u, d, shift):
    values = planes(u, 23, 18, slice(16, 40))
    return [residual_of(values, x + 1, d[24 + x, 16:40, :] - shift, 1, 1.0)[8:16] for x in range(CX)]


def mid_kernel(pos_ref, ag, wide, e, near, o, s, t, send_ref, d, u0n, b1n, u1n, stat_ref, u0, b1, u1, v1, pw, b2, u2, b3, u3, scr):
    total = ag[RING]
    for n in range(1, 32):
        total = total + ag[n * (RING + 1) + RING]
    total = jnp.sum(total)
    mean = total * (1.0 / COARSE_CELLS)
    for i in range(16):
        d[i] = jnp.zeros((W0Y, NZ), jnp.float32)
        d[48 + i] = jnp.zeros((W0Y, NZ), jnp.float32)
    d[:, 24:32, :] = wide[...]

    def place_first(e_row, o_row):
        d[:, e_row : e_row + 8, :] = e[...]
        d[0:16, o_row : o_row + 8, :] = o[0:16]
        d[16:48, o_row : o_row + 8, :] = near[...]
        d[48:64, o_row : o_row + 8, :] = o[16:32]

    def place_second(s_row, o_row):
        d[8:56, s_row : s_row + 8, :] = s[0:48]
        d[8:56, o_row : o_row + 8, :] = o[32:80]

    def place_third(s_row, t_row):
        d[16:48, s_row : s_row + 8, :] = s[48:80]
        d[16:48, t_row : t_row + 8, :] = t[...]

    even = (pos_ref[1] & 1) == 0
    for offset, place in ((8, place_first), (16, place_second), (24, place_third)):
        pl.when(even)(functools.partial(place, 24 + offset, 24 - offset))
        pl.when(jnp.logical_not(even))(functools.partial(place, 24 - offset, 24 + offset))
    clear(u0, 0, W0X - 1)
    first_sweep(u0, d, row_parity(W0Y, 1), 1, 1.0, 1, W0X - 1)
    clear(scr, *range(8))
    clear(b1, 0, W1X - 1)
    clear(u1, 0, W1X - 1)
    restrict_to(b1, u0, d, 0.0, W0Y, 1, 1.0, 1, W1X - 1, scr, W1Y)
    first_sweep(u1, b1, row_parity(W1Y, 2), 2, 4.0, 1, W1X - 1)
    coarse_solve(pos_ref, ag, mean, pw, b2, u2, b3, u3, scr)
    up_level1(v1, u1, b1, mean, u2, scr, 0, W1X, 0, W1Y)
    up_level0(u0n, u0, d, mean, mean * (1.0 / 3.0), v1, scr, 8, 56, 8, 40)
    stat_ref[0:8, :] = sum(r * r for r in own_residual(u0n, d, mean))
    stat_ref[8:16, :] = jnp.full((8, NZ), mean, jnp.float32)
    par0 = row_parity(40, 1)
    for colour in (0, 1):
        half_sweep(u0n, d, mean, par0, colour, 1, 1.0, 10, 54, 8)
    clear(scr, *range(RESTRICT))
    clear(b1n, *range(6), *range(26, W1X))
    restrict_to(b1n, u0n, d, mean, 40, 1, 1.0, 6, 26, scr, W1Y, 8)
    clear(u1n, 0, W1X - 1)
    first_sweep(u1n, b1n, row_parity(W1Y, 2), 2, 4.0, 1, W1X - 1)
    own_coarse(u1n, b1n, send_ref, W1Y, 12, 12)


def post_kernel(pos_ref, ag, d, u0, b1, u1, stat, pot_ref, res_ref, sums_ref, v0, v1, pw, b2, u2, b3, u3, scr):
    mean = jnp.max(stat[8:16, :])
    coarse_solve(pos_ref, ag, 0.0, pw, b2, u2, b3, u3, scr)
    up_level1(v1, u1, b1, 0.0, u2, scr, 8, 24, 8, 16)
    up_level0(v0, u0, d, mean, 0.0, v1, scr, 20, 44, 16, 24)
    inv = 1.0 / jnp.full((CY, NZ), mean, jnp.float32)
    total = jnp.zeros((CY, NZ), jnp.float32)
    for i, r in enumerate(own_residual(v0, d, mean)):
        r = r * inv
        total = total + r * r
        res_ref[i] = -r
        pot_ref[i] = v0[24 + i, 24:32, :] * (-coupling * inv)
    first = stat[0:8, :] * (inv * inv)
    lane = lax.broadcasted_iota(jnp.int32, (1, NZ), 1)
    both = jnp.where(lane == 0, jnp.sum(first), 0.0) + jnp.where(lane == 1, jnp.sum(total), 0.0)
    for k in range(sums_ref.shape[0]):
        sums_ref[k] = both


def f32(*shape):
    return jax.ShapeDtypeStruct(shape, jnp.float32)


def kept(*shape):
    return pltpu.VMEM(shape, jnp.float32) if KEEP else f32(*shape)


def resident(x):
    return pltpu.with_memory_space_constraint(x, pltpu.VMEM) if KEEP else x


def vmem(*shape):
    return pltpu.VMEM(shape, jnp.float32)


COARSE_SCRATCH = (vmem(9, W2Y, NZ), vmem(W2X, W2Y, NZ), vmem(W2X, W2Y, NZ), vmem(W3X, W3Y, NZ), vmem(W3X, W3Y, NZ), vmem(8, 64, NZ))
LEVELS_OUT = (kept(W0X, W0Y, NZ), kept(W1X, W1Y, NZ), kept(W1X, W1Y, NZ))


def call(kernel, outs, scratch, *args, pos=None):
    whole = pl.BlockSpec(memory_space=VMEM)
    specs = [whole] * len(args)
    args = tuple(resident(a) for a in args)
    if pos is not None:
        specs = [pl.BlockSpec(memory_space=pltpu.SMEM)] + specs
        args = (pos, *args)
    return pl.pallas_call(
        kernel,
        out_shape=outs,
        in_specs=specs,
        out_specs=jax.tree.map(lambda _: whole, outs),
        scratch_shapes=list(scratch),
        compiler_params=pltpu.CompilerParams(vmem_limit_bytes=24 * 1024 * 1024),
    )(*args)


def pairs(count, step, chosen):
    both = []
    for i in range(count):
        if chosen(i):
            both += [(i, (i + step) % count), ((i + step) % count, i)]
    return both


def swap(x, axis, step, chosen):
    return lax.ppermute(x, axis, pairs(lax.axis_size(axis), step, chosen))


def even(i):
    return i % 2 == 0


def odd(i):
    return i % 2 == 1


def gather_all(block, pos):
    ring = resident(lax.all_to_all(block, Z_RING, 0, 0))
    copies = call(fan_kernel, kept(32, RING + 1, 2, NZ), (), ring, pos=pos)
    return lax.all_to_all(copies, PLANE, 0, 0).reshape(32 * (RING + 1), 2, NZ)


def x_window(d):
    first = lax.axis_index("gx_2") == 0
    partner = swap(d, GX, 1, even)
    chip = jnp.where(first, jnp.concatenate([d, partner]), jnp.concatenate([partner, d]))
    far = swap(jnp.where(first, chip[:24], chip[8:]), GX, 1, odd)
    near = swap(jnp.where(first, chip[24:], chip[:8]), GX, 3, even)
    return jnp.where(first, jnp.concatenate([far, chip, near]), jnp.concatenate([near, chip, far]))


def per_device(particle_cell, particle_mass):
    tile_x = lax.axis_index(GX)
    tile_y = lax.axis_index(GY)
    pos = jnp.stack([tile_x, tile_y]).astype(jnp.int32)
    cells = particle_cell.reshape(512, 128)
    masses = particle_mass.reshape(512, 128)
    density = call(deposit_kernel, kept(128, 128), (), cells, masses).reshape(CX, CY, NZ)
    wide = x_window(density)
    e = swap(wide, GY, 1, even)
    near = swap(wide[16:48], GY, 1, odd)
    outer = jnp.concatenate([wide[:16], wide[48:], e[8:56]])
    reach = jnp.concatenate([e[8:56], wide[16:48]])
    send = call(
        send_kernel,
        kept(16, 2, NZ),
        (vmem(32, 24, NZ), vmem(32, 24, NZ), vmem(16, 16, NZ), vmem(16, 16, NZ), vmem(8, 64, NZ)),
        wide, e, near,
        pos=pos,
    )
    got = gather_all(send, pos)
    o = swap(outer, GY, 1, odd)
    s = swap(reach, GY, 3, even)
    t = swap(wide[16:48], GY, 3, odd)
    send, d, u0, b1, u1, stat = call(
        mid_kernel,
        (kept(16, 2, NZ), kept(W0X, W0Y, NZ), *LEVELS_OUT, kept(16, NZ)),
        (vmem(W0X, W0Y, NZ), vmem(W1X, W1Y, NZ), vmem(W1X, W1Y, NZ), vmem(W1X, W1Y, NZ), *COARSE_SCRATCH),
        got, wide, e, near, o, s, t,
        pos=pos,
    )
    got = gather_all(send, pos)
    potential, residual, sums = call(
        post_kernel,
        (f32(CX, CY, NZ), f32(CX, CY, NZ), kept(16, 1, NZ)),
        (vmem(W0X, W0Y, NZ), vmem(W1X, W1Y, NZ), *COARSE_SCRATCH),
        got, d, u0, b1, u1, stat,
        pos=pos,
    )
    ring = jnp.sum(lax.all_to_all(sums, Z_RING, 0, 0), axis=0)
    total = jnp.sum(lax.all_to_all(jnp.broadcast_to(ring[None], (32, 1, NZ)), PLANE, 0, 0), axis=(0, 1))
    norms = jnp.sqrt(total[:2] / GRID_CELLS + norm_eps)
    return potential, residual, norms


def solution(mesh):
    split = Mesh(mesh.devices.reshape(2, 4, 2, 8, 4), ("gx_0", "gx_1", "gx_2", "gy_0", "gy_1"))
    placed = (P(GX, GY, None), P(GX, GY, None))
    return jax.shard_map(
        per_device,
        mesh=split,
        in_specs=placed,
        out_specs=(P(GX, GY, None), P(GX, GY, None), P()),
        check_vma=False,
    )
```

```python
import functools

import jax
import jax.numpy as jnp
from jax import lax
from jax.experimental import pallas as pl
from jax.experimental.pallas import tpu as pltpu
from jax.sharding import Mesh
from jax.sharding import PartitionSpec as P


CX = 16
CY = 8
NZ = 128
GX = ("gx_0", "gx_1", "gx_2")
GY = ("gy_0", "gy_1")
Z_RING = ("gx_0", "gy_0")
PLANE = ("gx_1", "gx_2", "gy_1")
TILES_X = 16
TILES_Y = 32
GRID_CELLS = 256 * 256 * 128
COARSE_CELLS = 64 * 64 * 32

coupling = 0.03125
norm_eps = 1e-06

W0X, W0Y = 64, 56
W1X, W1Y = 32, 32
W2X, W2Y = 36, 40
W3X, W3Y = 18, 24
DEPOSIT_ROWS = 64
KEEP = True
RING = 10
RESTRICT = 4
ADD = 4
SIZES = (6, 8, 10, 16, 16)
VMEM = pltpu.VMEM


def deposit_kernel(cell_ref, mass_ref, out_ref):
    rows = lax.broadcasted_iota(jnp.int32, (128, 128), 0).astype(jnp.bfloat16)
    batch = DEPOSIT_ROWS

    def step(t, acc):
        cells = cell_ref[pl.ds(pl.multiple_of(t * batch, 8), batch), :]
        masses = mass_ref[pl.ds(pl.multiple_of(t * batch, 8), batch), :]
        high = (cells >> 7).astype(jnp.bfloat16)
        low = (cells & 127).astype(jnp.bfloat16)
        coarse = masses.astype(jnp.bfloat16)
        fine = (masses - coarse.astype(jnp.float32)).astype(jnp.bfloat16)
        zero = jnp.zeros((128, 128), jnp.bfloat16)
        one = jnp.ones((128, 128), jnp.bfloat16)
        left, right = [], []
        for r in range(batch):
            line = lambda x: jnp.broadcast_to(x[r : r + 1, :], (128, 128))
            hit = rows == line(high)
            left.append(jnp.concatenate([jnp.where(hit, line(coarse), zero), jnp.where(hit, line(fine), zero)], axis=0))
            right.append(jnp.where(rows == line(low), one, zero))
        left = jnp.concatenate(left, axis=1)
        right = jnp.concatenate(right, axis=1)
        return acc + lax.dot_general(left, right, (((1,), (1,)), ((), ())), preferred_element_type=jnp.float32)

    total = lax.fori_loop(0, cell_ref.shape[0] // batch, step, jnp.zeros((256, 128), jnp.float32))
    out_ref[...] = total[:128] + total[128:]


def row_parity(rows, lanes_per_cell, extra=0):
    j = lax.broadcasted_iota(jnp.int32, (rows, NZ), 0)
    z = lax.broadcasted_iota(jnp.int32, (rows, NZ), 1) // lanes_per_cell
    return (j + z + extra) & 1


def batched(lo, hi, size, body):
    size = min(size, hi - lo)
    runs = -(-(hi - lo) // size)
    if runs == 1:
        body(lo, size)
        return

    def step(t, carry):
        body(jnp.minimum(lo + t * size, hi - size), size)
        return carry

    lax.fori_loop(0, runs, step, 0)


def batch_of(rows):
    return {56: SIZES[0], 40: SIZES[1], 32: SIZES[2], 24: SIZES[3], 16: SIZES[4]}[rows]


def planes(ref, first, count, part):
    return [ref[first + j, part, :] for j in range(count)]


def neighbours(values, j, lanes):
    c = values[j]
    rows = c.shape[0]
    n = values[j - 1] + values[j + 1]
    n = n + (pltpu.roll(c, 1, 0) + pltpu.roll(c, rows - 1, 0))
    return c, n + (pltpu.roll(c, lanes, 1) + pltpu.roll(c, NZ - lanes, 1))


def pair_z(t, lanes):
    z = lax.broadcasted_iota(jnp.int32, t.shape, 1) // lanes
    return t + jnp.where((z & 1) == 0, pltpu.roll(t, NZ - lanes, 1), pltpu.roll(t, lanes, 1))


def first_sweep(u, b, parity, lanes, s, lo, hi):
    rows = parity.shape[0]
    red = (parity == 0, parity == 1)

    def body(first, count):
        values = planes(b, first - 1, count + 2, slice(0, rows))
        for j in range(count):
            c, n = neighbours(values, j + 1, lanes)
            own = c * (s / 6.0)
            u[first + j, 0:rows, :] = jnp.where(red[(lo + j) & 1], own, n * (s / 36.0) + own)

    batched(lo, hi, batch_of(rows), body)


def half_sweep(u, b, shift, parity, colour, lanes, s, lo, hi, top=0):
    rows = parity.shape[0]
    part = slice(top, top + rows)
    chosen = (parity == (colour & 1), parity == ((1 + colour) & 1))

    def body(first, count):
        values = planes(u, first - 1, count + 2, part)
        made = []
        for j in range(count):
            c, n = neighbours(values, j + 1, lanes)
            rhs = (b[first + j, part, :] - shift) * (s / 6.0)
            made.append(jnp.where(chosen[(lo + j) & 1], n * (1.0 / 6.0) + rhs, c))
        for j in range(count):
            u[first + j, part, :] = made[j]

    batched(lo, hi, batch_of(rows), body)


def residual_of(values, j, b, lanes, s):
    c, n = neighbours(values, j, lanes)
    return b - (6.0 * c - n) * (1.0 / s)


def restrict_to(out, u, b, shift, rows, lanes, s, lo, hi, scr, out_rows, top=0):
    part = slice(top, top + rows)

    def body(first, count):
        values = planes(u, 2 * first - 1, 2 * count + 2, part)
        for k in range(count):
            t = residual_of(values, 2 * k + 1, b[2 * (first + k), part, :] - shift, lanes, s)
            t = t + residual_of(values, 2 * k + 2, b[2 * (first + k) + 1, part, :] - shift, lanes, s)
            scr[k, part, :] = pair_z(t, lanes)
        for k in range(count):
            out[first + k] = (scr.at[k][pl.ds(0, out_rows, 2), :] + scr.at[k][pl.ds(1, out_rows, 2), :]) * 0.125

    batched(lo, hi, RESTRICT, body)


def add_coarse(fine, base, shift, coarse, offset, first_row, half, lo, hi, top, rows, scr):
    part = slice(top, top + rows)

    def body(first, count):
        for k in range(count):
            c = coarse[first + k + offset, first_row : first_row + half, :]
            scr.at[k][pl.ds(0, half, 2), :] = c
            scr.at[k][pl.ds(1, half, 2), :] = c
        for k in range(count):
            c = scr[k, 0:rows, :] - shift
            i = 2 * (first + k)
            even, odd = base[i, part, :] + c, base[i + 1, part, :] + c
            fine[i, part, :] = even
            fine[i + 1, part, :] = odd

    batched(lo, hi, (hi - lo) // 2 if base is fine else ADD, body)


def own_coarse(u1, b1, send_ref, rows, plane, row):
    lane = lax.broadcasted_iota(jnp.int32, (rows, NZ), 1) & 3
    packed = jnp.zeros((rows, NZ), jnp.float32)
    values = planes(u1, plane - 1, 10, slice(0, rows))
    for x in range(4):
        i = plane + 2 * x
        t = residual_of(values, 2 * x + 1, b1[i, 0:rows, :], 2, 4.0)
        t = t + residual_of(values, 2 * x + 2, b1[i + 1, 0:rows, :], 2, 4.0)
        t = pair_z(t, 2)
        t = (t + pltpu.roll(t, rows - 1, 0)) * 0.125
        packed = jnp.where(lane == x, t, packed)
    for k in range(send_ref.shape[0]):
        send_ref[k, 0:1, :] = packed[row : row + 1, :]
        send_ref[k, 1:2, :] = packed[row + 2 : row + 3, :]


def clear(ref, *indices):
    for i in indices:
        ref[i] = jnp.zeros(ref.shape[1:], jnp.float32)


def fan_kernel(pos_ref, ring, *rest):
    out = rest[-1]
    block = lax.shift_right_logical(pos_ref[1], 2)
    parts = [ring[8 * h + ((block + (j + 6)) & 7)] for h in range(2) for j in range(5)]
    parts.append(jnp.sum(ring[...], axis=0))
    for n in range(32):
        for j in range(RING + 1):
            out[n, j] = parts[j]


def coarse_solve(pos_ref, ag, shift, pw, b2, u2, b3, u3, scr):
    gx, gy = pos_ref[0], pos_ref[1]
    for tx in range(9):
        pw[tx, 32:40, :] = jnp.zeros((8, NZ), jnp.float32)
        x = lax.rem(gx + (tx - 4 + TILES_X), TILES_X)
        for ty in range(17):
            y = lax.rem(gy + (ty - 8 + TILES_Y), TILES_Y)
            plane = (x & 7) * 4 + (y & 3)
            ring = (x >> 3) * 5 + (((y >> 2) - (gy >> 2) + 2) & 7)
            pw[tx, 2 * ty : 2 * ty + 2, :] = ag[plane * (RING + 1) + ring]
    lane = lax.broadcasted_iota(jnp.int32, (W2Y, NZ), 1) & 3

    def unpack(first, count):
        for k in range(count):
            t = pw[first + k]
            for j in range(4):
                v = jnp.where(lane == j, t, 0.0)
                v = v + pltpu.roll(v, 1 if j % 2 == 0 else NZ - 1, 1)
                v = v + pltpu.roll(v, 2 if j < 2 else NZ - 2, 1)
                b2[4 * (first + k) + j] = v - shift

    batched(0, 9, 3, unpack)
    par2 = row_parity(W2Y, 4)
    clear(u2, 0, W2X - 1)
    first_sweep(u2, b2, par2, 4, 16.0, 1, W2X - 1)
    clear(scr, *range(RESTRICT))
    clear(b3, 0, W3X - 1)
    clear(u3, 0, W3X - 1)
    restrict_to(b3, u2, b2, 0.0, W2Y, 4, 16.0, 1, W3X - 1, scr, W3Y)
    par3 = row_parity(W3Y, 8, gy)
    first_sweep(u3, b3, par3, 8, 64.0, 1, W3X - 1)
    for colour in (0, 1):
        half_sweep(u3, b3, 0.0, par3, colour, 8, 64.0, 2, W3X - 2)
    add_coarse(u2, u2, 0.0, u3, 0, 0, W3Y, 4, 14, 0, W2Y, scr)
    half_sweep(u2, b2, 0.0, par2, 0, 4, 16.0, 9, 27)
    half_sweep(u2, b2, 0.0, par2, 1, 4, 16.0, 10, 26)


def up_level1(v1, u1, b1, shift, u2, scr, lo, hi, top, rows):
    add_coarse(v1, u1, shift * (4.0 / 3.0), u2, 10, 10 + top // 2, rows // 2, lo // 2, hi // 2, top, rows, scr)
    par1 = row_parity(rows, 2)
    for colour in (0, 1):
        half_sweep(v1, b1, shift, par1, colour, 2, 4.0, lo + 1, hi - 1, top)


def up_level0(v0, u0, d, shift, base, v1, scr, lo, hi, top, rows):
    half = (rows // 2 + 7) // 8 * 8
    add_coarse(v0, u0, base, v1, 0, top // 2, half, lo // 2, hi // 2, top, rows, scr)
    par0 = row_parity(rows, 1)
    for colour in (0, 1):
        half_sweep(v0, d, shift, par0, colour, 1, 1.0, lo + 1, hi - 1, top)


def beside(pos_ref, place, own):
    even = (pos_ref[1] & 1) == 0
    pl.when(even)(functools.partial(place, own + 8, own - 8))
    pl.when(jnp.logical_not(even))(functools.partial(place, own - 8, own + 8))


def send_kernel(pos_ref, wide, e, near, send_ref, d, u0, b1, u1, scr):
    d[:, 8:16, :] = wide[16:48]

    def place(e_row, o_row):
        d[:, e_row : e_row + 8, :] = e[16:48]
        d[:, o_row : o_row + 8, :] = near[...]

    beside(pos_ref, place, 8)
    clear(u0, 0, 31)
    first_sweep(u0, d, row_parity(24, 1), 1, 1.0, 1, 31)
    clear(scr, *range(RESTRICT))
    clear(b1, 0, 15)
    clear(u1, 0, 15)
    restrict_to(b1, u0, d, 0.0, 24, 1, 1.0, 1, 15, scr, 16)
    first_sweep(u1, b1, row_parity(16, 2), 2, 4.0, 1, 15)
    own_coarse(u1, b1, send_ref, 16, 4, 4)


def own_residual(u, d, shift):
    values = planes(u, 23, 18, slice(16, 40))
    return [residual_of(values, x + 1, d[24 + x, 16:40, :] - shift, 1, 1.0)[8:16] for x in range(CX)]


def mid_kernel(pos_ref, ag, wide, e, near, o, s, t, send_ref, d, u0n, b1n, u1n, stat_ref, u0, b1, u1, v1, pw, b2, u2, b3, u3, scr):
    total = ag[RING]
    for n in range(1, 32):
        total = total + ag[n * (RING + 1) + RING]
    total = jnp.sum(total)
    mean = total * (1.0 / COARSE_CELLS)
    for i in range(16):
        d[i] = jnp.zeros((W0Y, NZ), jnp.float32)
        d[48 + i] = jnp.zeros((W0Y, NZ), jnp.float32)
    d[:, 24:32, :] = wide[...]

    def place_first(e_row, o_row):
        d[:, e_row : e_row + 8, :] = e[...]
        d[0:16, o_row : o_row + 8, :] = o[0:16]
        d[16:48, o_row : o_row + 8, :] = near[...]
        d[48:64, o_row : o_row + 8, :] = o[16:32]

    def place_second(s_row, o_row):
        d[8:56, s_row : s_row + 8, :] = s[0:48]
        d[8:56, o_row : o_row + 8, :] = o[32:80]

    def place_third(s_row, t_row):
        d[16:48, s_row : s_row + 8, :] = s[48:80]
        d[16:48, t_row : t_row + 8, :] = t[...]

    even = (pos_ref[1] & 1) == 0
    for offset, place in ((8, place_first), (16, place_second), (24, place_third)):
        pl.when(even)(functools.partial(place, 24 + offset, 24 - offset))
        pl.when(jnp.logical_not(even))(functools.partial(place, 24 - offset, 24 + offset))
    clear(u0, 0, W0X - 1)
    first_sweep(u0, d, row_parity(W0Y, 1), 1, 1.0, 1, W0X - 1)
    clear(scr, *range(8))
    clear(b1, 0, W1X - 1)
    clear(u1, 0, W1X - 1)
    restrict_to(b1, u0, d, 0.0, W0Y, 1, 1.0, 1, W1X - 1, scr, W1Y)
    first_sweep(u1, b1, row_parity(W1Y, 2), 2, 4.0, 1, W1X - 1)
    coarse_solve(pos_ref, ag, mean, pw, b2, u2, b3, u3, scr)
    up_level1(v1, u1, b1, mean, u2, scr, 0, W1X, 0, W1Y)
    up_level0(u0n, u0, d, mean, mean * (1.0 / 3.0), v1, scr, 8, 56, 8, 40)
    stat_ref[0:8, :] = sum(r * r for r in own_residual(u0n, d, mean))
    stat_ref[8:16, :] = jnp.full((8, NZ), mean, jnp.float32)
    par0 = row_parity(40, 1)
    for colour in (0, 1):
        half_sweep(u0n, d, mean, par0, colour, 1, 1.0, 10, 54, 8)
    clear(scr, *range(RESTRICT))
    clear(b1n, *range(6), *range(26, W1X))
    restrict_to(b1n, u0n, d, mean, 40, 1, 1.0, 6, 26, scr, W1Y, 8)
    clear(u1n, 0, W1X - 1)
    first_sweep(u1n, b1n, row_parity(W1Y, 2), 2, 4.0, 1, W1X - 1)
    own_coarse(u1n, b1n, send_ref, W1Y, 12, 12)


def post_kernel(pos_ref, ag, d, u0, b1, u1, stat, pot_ref, res_ref, sums_ref, v0, v1, pw, b2, u2, b3, u3, scr):
    mean = jnp.max(stat[8:16, :])
    coarse_solve(pos_ref, ag, 0.0, pw, b2, u2, b3, u3, scr)
    up_level1(v1, u1, b1, 0.0, u2, scr, 8, 24, 8, 16)
    up_level0(v0, u0, d, mean, 0.0, v1, scr, 20, 44, 16, 24)
    inv = 1.0 / jnp.full((CY, NZ), mean, jnp.float32)
    total = jnp.zeros((CY, NZ), jnp.float32)
    for i, r in enumerate(own_residual(v0, d, mean)):
        r = r * inv
        total = total + r * r
        res_ref[i] = -r
        pot_ref[i] = v0[24 + i, 24:32, :] * (-coupling * inv)
    first = stat[0:8, :] * (inv * inv)
    lane = lax.broadcasted_iota(jnp.int32, (1, NZ), 1)
    both = jnp.where(lane == 0, jnp.sum(first), 0.0) + jnp.where(lane == 1, jnp.sum(total), 0.0)
    for k in range(sums_ref.shape[0]):
        sums_ref[k] = both


def f32(*shape):
    return jax.ShapeDtypeStruct(shape, jnp.float32)


def kept(*shape):
    return pltpu.VMEM(shape, jnp.float32) if KEEP else f32(*shape)


def resident(x):
    return pltpu.with_memory_space_constraint(x, pltpu.VMEM) if KEEP else x


def vmem(*shape):
    return pltpu.VMEM(shape, jnp.float32)


COARSE_SCRATCH = (vmem(9, W2Y, NZ), vmem(W2X, W2Y, NZ), vmem(W2X, W2Y, NZ), vmem(W3X, W3Y, NZ), vmem(W3X, W3Y, NZ), vmem(8, 64, NZ))
LEVELS_OUT = (kept(W0X, W0Y, NZ), kept(W1X, W1Y, NZ), kept(W1X, W1Y, NZ))


def call(kernel, outs, scratch, *args, pos=None):
    whole = pl.BlockSpec(memory_space=VMEM)
    specs = [whole] * len(args)
    args = tuple(resident(a) for a in args)
    if pos is not None:
        specs = [pl.BlockSpec(memory_space=pltpu.SMEM)] + specs
        args = (pos, *args)
    return pl.pallas_call(
        kernel,
        out_shape=outs,
        in_specs=specs,
        out_specs=jax.tree.map(lambda _: whole, outs),
        scratch_shapes=list(scratch),
        compiler_params=pltpu.CompilerParams(vmem_limit_bytes=24 * 1024 * 1024),
    )(*args)


def pairs(count, step, chosen):
    both = []
    for i in range(count):
        if chosen(i):
            both += [(i, (i + step) % count), ((i + step) % count, i)]
    return both


def swap(x, axis, step, chosen):
    return lax.ppermute(x, axis, pairs(lax.axis_size(axis), step, chosen))


def even(i):
    return i % 2 == 0


def odd(i):
    return i % 2 == 1


def gather_all(block, pos, *held):
    ring = resident(lax.all_to_all(block, Z_RING, 0, 0))
    copies = call(fan_kernel, kept(32, RING + 1, 2, NZ), (), ring, *held, pos=pos)
    return lax.all_to_all(copies, PLANE, 0, 0).reshape(32 * (RING + 1), 2, NZ)


def x_window(d):
    first = lax.axis_index("gx_2") == 0
    partner = swap(d, GX, 1, even)
    chip = jnp.where(first, jnp.concatenate([d, partner]), jnp.concatenate([partner, d]))
    far = swap(jnp.where(first, chip[:24], chip[8:]), GX, 1, odd)
    near = swap(jnp.where(first, chip[24:], chip[:8]), GX, 3, even)
    return jnp.where(first, jnp.concatenate([far, chip, near]), jnp.concatenate([near, chip, far]))


def per_device(particle_cell, particle_mass):
    tile_x = lax.axis_index(GX)
    tile_y = lax.axis_index(GY)
    pos = jnp.stack([tile_x, tile_y]).astype(jnp.int32)
    cells = particle_cell.reshape(512, 128)
    masses = particle_mass.reshape(512, 128)
    density = call(deposit_kernel, kept(128, 128), (), cells, masses).reshape(CX, CY, NZ)
    wide = x_window(density)
    near = swap(wide[16:48], GY, 1, odd)
    e = swap(wide, GY, 1, even)
    outer = jnp.concatenate([wide[:16], wide[48:], e[8:56]])
    reach = jnp.concatenate([e[8:56], wide[16:48]])
    send = call(
        send_kernel,
        kept(16, 2, NZ),
        (vmem(32, 24, NZ), vmem(32, 24, NZ), vmem(16, 16, NZ), vmem(16, 16, NZ), vmem(8, 64, NZ)),
        wide, e, near,
        pos=pos,
    )
    s = swap(reach, GY, 3, even)
    t = swap(wide[16:48], GY, 3, odd)
    got = gather_all(send, pos, s, t)
    o = swap(outer, GY, 1, odd)
    send, d, u0, b1, u1, stat = call(
        mid_kernel,
        (kept(16, 2, NZ), kept(W0X, W0Y, NZ), *LEVELS_OUT, kept(16, NZ)),
        (vmem(W0X, W0Y, NZ), vmem(W1X, W1Y, NZ), vmem(W1X, W1Y, NZ), vmem(W1X, W1Y, NZ), *COARSE_SCRATCH),
        got, wide, e, near, o, s, t,
        pos=pos,
    )
    got = gather_all(send, pos)
    potential, residual, sums = call(
        post_kernel,
        (f32(CX, CY, NZ), f32(CX, CY, NZ), kept(16, 1, NZ)),
        (vmem(W0X, W0Y, NZ), vmem(W1X, W1Y, NZ), *COARSE_SCRATCH),
        got, d, u0, b1, u1, stat,
        pos=pos,
    )
    ring = jnp.sum(lax.all_to_all(sums, Z_RING, 0, 0), axis=0)
    total = jnp.sum(lax.all_to_all(jnp.broadcast_to(ring[None], (32, 1, NZ)), PLANE, 0, 0), axis=(0, 1))
    norms = jnp.sqrt(total[:2] / GRID_CELLS + norm_eps)
    return potential, residual, norms


def solution(mesh):
    split = Mesh(mesh.devices.reshape(2, 4, 2, 8, 4), ("gx_0", "gx_1", "gx_2", "gy_0", "gy_1"))
    placed = (P(GX, GY, None), P(GX, GY, None))
    return jax.shard_map(
        per_device,
        mesh=split,
        in_specs=placed,
        out_specs=(P(GX, GY, None), P(GX, GY, None), P()),
        check_vma=False,
    )
```
